32 devices in a mesh: dp: 1 (over z), ep: 32 (over y, x, core).
Axes of the slice: x: 4, y: 4, z: 1, core: 2. Of those that a mesh axis runs over, the one named last changes fastest.
The devices are a block of a 4x4x8 slice.
Arguments:
- tok_x: bfloat16 [32768, 1024], P(('dp', 'ep'))
- expert_ids: int32 [32768, 8], P(('dp', 'ep'))
- gates: float32 [32768, 8], P(('dp', 'ep'))
- hot_tok: int32 [32768], P(('dp', 'ep'))
- hot_gates: float32 [32768], P(('dp', 'ep'))
- w_gate: bfloat16 [32, 1024, 512], P('ep')
- w_up: bfloat16 [32, 1024, 512], P('ep')
- w_down: bfloat16 [32, 512, 1024], P('ep')
Outputs:
- output: bfloat16 [32768, 1024], P(('dp', 'ep'))
All inputs are finite; a program needn't handle non-finite values.
Results may differ from the reference program's by a relative error of at most 0.00796467.
Values are sent between devices in bfloat16 or wider.
A program may use at most 768 MiB of HBM per device.

```python
import jax
import jax.numpy as jnp
from jax import lax

GROUP_SIZE = 32
TOKENS = 1024
D_MODEL = 1024
D_FF = 512
EXPERTS = 32
TOP_K = 8
HOT_ROWS = 1024

COLD_CAP = (TOKENS * TOP_K + EXPERTS - 2) // (EXPERTS - 1)


def draw_routing(key):
    key_rows, key_label, key_hot = jax.random.split(key, 3)
    row_perm = jax.random.permutation(key_rows, TOKENS)
    label_perm = jax.random.permutation(key_label, EXPERTS - 1)
    route_num = (row_perm[:, None] * TOP_K + jnp.arange(TOP_K)[None, :]) % (EXPERTS - 1)
    chip_ids = 1 + label_perm[route_num]
    hot_list = jax.random.permutation(key_hot, TOKENS)[:HOT_ROWS]
    return chip_ids.astype(jnp.int32), hot_list.astype(jnp.int32)


def setup_inputs(seed: int = 0, part: int = 0) -> dict:
    base_key = jax.random.key(seed)
    key_wg, key_wu, key_wd = jax.random.split(base_key, 3)
    part_key = jax.random.fold_in(base_key, part)
    key_x, key_route, key_gate, key_hot = jax.random.split(part_key, 4)
    row_count = GROUP_SIZE * TOKENS
    tok_x = jax.random.normal(key_x, (row_count, D_MODEL), jnp.float32).astype(jnp.bfloat16)
    chip_ids, hot_list = jax.vmap(draw_routing)(jax.random.split(key_route, GROUP_SIZE))
    gates = jax.random.uniform(key_gate, (row_count, TOP_K), jnp.float32, 0.5, 1.5) * TOP_K ** -0.5
    hot_gates = jax.random.uniform(key_hot, (GROUP_SIZE * HOT_ROWS,), jnp.float32, 0.5, 1.5)
    w_gate = (jax.random.normal(key_wg, (EXPERTS, D_MODEL, D_FF), jnp.float32) * D_MODEL ** -0.5).astype(jnp.bfloat16)
    w_up = (jax.random.normal(key_wu, (EXPERTS, D_MODEL, D_FF), jnp.float32) * D_MODEL ** -0.5).astype(jnp.bfloat16)
    w_down = (jax.random.normal(key_wd, (EXPERTS, D_FF, D_MODEL), jnp.float32) * D_FF ** -0.5).astype(jnp.bfloat16)
    return {'tok_x': tok_x, 'expert_ids': chip_ids.reshape(row_count, TOP_K), 'gates': gates,
            'hot_tok': hot_list.reshape(GROUP_SIZE * HOT_ROWS), 'hot_gates': hot_gates,
            'w_gate': w_gate, 'w_up': w_up, 'w_down': w_down}


def swiglu_rows(in_rows, w_gate_e, w_up_e, w_down_e):
    gate_act = jnp.dot(in_rows, w_gate_e, preferred_element_type=jnp.float32)
    up_act = jnp.dot(in_rows, w_up_e, preferred_element_type=jnp.float32)
    hidden = (jax.nn.silu(gate_act) * up_act).astype(jnp.bfloat16)
    return jnp.dot(hidden, w_down_e, preferred_element_type=jnp.float32).astype(jnp.bfloat16)


def reference(tok_x, expert_ids, gates, hot_tok, hot_gates, w_gate, w_up, w_down):
    routes = GROUP_SIZE * TOKENS * TOP_K
    flat_ids = expert_ids.reshape(routes)
    flat_gates = gates.reshape(routes)
    max_rows = GROUP_SIZE * COLD_CAP

    def expert_step(y_sum, expert_args):
        expert, w_gate_e, w_up_e, w_down_e = expert_args
        found_pos = jnp.nonzero(flat_ids == expert, size=max_rows, fill_value=routes)[0]
        in_range = found_pos < routes
        safe_pos = jnp.minimum(found_pos, routes - 1)
        tok_rows = safe_pos // TOP_K
        weight = jnp.where(in_range, flat_gates[safe_pos], 0.0)
        expert_out = swiglu_rows(tok_x[tok_rows], w_gate_e, w_up_e, w_down_e)
        y_sum = y_sum.at[tok_rows].add(weight[:, None] * expert_out.astype(jnp.float32))
        return y_sum, None

    y_start = jnp.zeros((GROUP_SIZE * TOKENS, D_MODEL), jnp.float32)
    y_sum, unused = lax.scan(expert_step, y_start, (jnp.arange(EXPERTS, dtype=jnp.int32), w_gate, w_up, w_down))
    chip_base = (jnp.arange(GROUP_SIZE * HOT_ROWS, dtype=jnp.int32) // HOT_ROWS) * TOKENS
    hot_rows_idx = chip_base + hot_tok
    hot_out = swiglu_rows(tok_x[hot_rows_idx], w_gate[0], w_up[0], w_down[0])
    y_sum = y_sum.at[hot_rows_idx].add(hot_gates[:, None] * hot_out.astype(jnp.float32))
    return y_sum.astype(jnp.bfloat16)
```

```python
import functools

import jax
import jax.numpy as jnp
from jax import lax
from jax.experimental import pallas as pl
from jax.experimental.pallas import tpu as pltpu
from jax.sharding import PartitionSpec as P

MESH = pl.DeviceIdType.MESH
F32 = jnp.float32
BF16 = jnp.bfloat16
OFFSETS = ((0, 0), (1, 1), (3, 3), (1, 3), (3, 1), (2, 2), (1, 2), (3, 2), (2, 1), (2, 3),
           (1, 0), (3, 0), (0, 1), (0, 3), (2, 0), (0, 2))
SIDE = 4
HOT_STEP = 16
LAG = 2


def packed(values):
    return sum(v << (2 * i) for i, v in enumerate(values[1:]))


TABLE_X = packed([o[0] for o in OFFSETS])
TABLE_Y = packed([o[1] for o in OFFSETS])


def moe_kernel(n, cap_p, x_ref, ids_ref, gates_ref, hot_tok_ref, hot_g_ref, wg_ref, wu_ref, wd_ref, out_ref,
               own, hot, xbuf, hbuf, slot_t, gate_t, slot_r, hot_w, acc,
               w_sem, s1_send, s1_recv, s2_send, s2_recv, s3_send, s3_recv,
               x_send, x_recv, h_send, h_recv, free):
    tokens, d_model = x_ref.shape
    top_k = ids_ref.shape[1]
    d_ff = wg_ref.shape[2]
    lanes = slot_t.shape[1]
    chunk = own.shape[0] // n
    half = n // 2
    me = lax.axis_index('ep')
    core = lax.rem(me, 2)
    chip = lax.div(me, 2)
    px = lax.rem(chip, SIDE)
    py = lax.div(chip, SIDE)

    barrier = pltpu.get_barrier_semaphore()

    def greet(k, c):
        pl.semaphore_signal(barrier, inc=1, device_id={'ep': lax.rem(me + k, n)}, device_id_type=MESH)
        return c
    lax.fori_loop(1, n, greet, 0)

    w_copies = (
        pltpu.make_async_copy(wg_ref.at[0], own.at[pl.ds(0, d_model), pl.ds(0, d_ff)], w_sem.at[0]),
        pltpu.make_async_copy(wu_ref.at[0], own.at[pl.ds(0, d_model), pl.ds(d_ff, d_ff)], w_sem.at[1]),
        pltpu.make_async_copy(wd_ref.at[0], own.at[pl.ds(d_model, d_ff), :], w_sem.at[2]),
    )
    for copy in w_copies:
        copy.start()

    def shifted(q, sign):
        j = lax.div(q, 2)
        i = 2 * lax.max(j - 1, 0)
        near = lax.min(j, 1)
        dx = lax.rem(lax.shift_right_logical(jnp.int32(TABLE_X), i), SIDE) * near
        dy = lax.rem(lax.shift_right_logical(jnp.int32(TABLE_Y), i), SIDE) * near
        dc = lax.rem(q, 2)
        tx = lax.rem(px + sign * dx + SIDE, SIDE)
        ty = lax.rem(py + sign * dy + SIDE, SIDE)
        return (ty * SIDE + tx) * 2 + lax.rem(core + dc, 2)

    def x_copy(q):
        return pltpu.make_async_remote_copy(
            src_ref=xbuf.at[q], dst_ref=hbuf.at[q], send_sem=x_send.at[q], recv_sem=x_recv.at[q],
            device_id={'ep': shifted(q, 1)}, device_id_type=MESH)

    def h_copy(q):
        return pltpu.make_async_remote_copy(
            src_ref=hbuf.at[q], dst_ref=xbuf.at[q], send_sem=h_send.at[q], recv_sem=h_recv.at[q],
            device_id={'ep': shifted(q, -1)}, device_id_type=MESH)

    lane = lax.broadcasted_iota(jnp.int32, (tokens, lanes), 1)
    chosen = jnp.zeros((tokens, lanes), F32)
    gate_sum = jnp.zeros((tokens, lanes), F32)
    for j in range(top_k):
        hit = ids_ref[:, j:j + 1] == lane
        chosen = jnp.where(hit, 1.0, chosen)
        gate_sum = jnp.where(hit, gates_ref[:, j:j + 1], gate_sum)
    gate_t[...] = gate_sum
    chosen_b = chosen.astype(BF16)
    step = 256
    for r in range(tokens // step):
        rows = lax.broadcasted_iota(jnp.int32, (step, tokens), 0) + r * step
        before = jnp.where(lax.broadcasted_iota(jnp.int32, (step, tokens), 1) < rows, 1.0, 0.0).astype(BF16)
        rank = jnp.dot(before, chosen_b, preferred_element_type=F32)
        slot_t[pl.ds(r * step, step), :] = jnp.where(chosen[r * step:(r + 1) * step] > 0.5, rank, -1.0)
    slot_r[...] = slot_t[...].T

    pl.semaphore_wait(barrier, n - 1)

    for copy in w_copies:
        copy.wait()

    def piece(d):
        return pl.ds(pl.multiple_of((lax.rem(d, 2) * half + lax.div(d, 2)) * chunk, chunk), chunk)

    def s1_copy(d):
        return pltpu.make_async_remote_copy(
            src_ref=own.at[piece(d), :], dst_ref=hot.at[piece(d), :], send_sem=s1_send.at[d], recv_sem=s1_recv,
            device_id={'ep': d}, device_id_type=MESH)

    @pl.when(me == 0)
    def _():
        hot[pl.ds(0, chunk), :] = own[pl.ds(0, chunk), :]

        def send(d, c):
            s1_copy(d).start()
            return c
        lax.fori_loop(1, n, send, 0)

    def s2_copy(k):
        peer = lax.rem(chip + k, half) * 2 + core
        return pltpu.make_async_remote_copy(
            src_ref=hot.at[piece(me), :], dst_ref=hot.at[piece(me), :], send_sem=s2_send.at[k], recv_sem=s2_recv.at[k],
            device_id={'ep': peer}, device_id_type=MESH)

    def s2_arrival(k):
        peer = lax.rem(chip + half - k, half) * 2 + core
        return pltpu.make_async_remote_copy(
            src_ref=hot.at[piece(peer), :], dst_ref=hot.at[piece(peer), :], send_sem=s2_send.at[k],
            recv_sem=s2_recv.at[k], device_id={'ep': peer}, device_id_type=MESH)

    def core_half(c):
        return hot.at[pl.ds(pl.multiple_of(c * half * chunk, chunk), half * chunk), :]

    def s3_copy(c):
        return pltpu.make_async_remote_copy(
            src_ref=core_half(c), dst_ref=core_half(c), send_sem=s3_send, recv_sem=s3_recv,
            device_id={'ep': chip * 2 + 1 - core}, device_id_type=MESH)

    def gather(q):
        place = slot_r[pl.ds(shifted(q, 1), 1), :]
        pos = lax.broadcasted_iota(jnp.int32, (cap_p, tokens), 0).astype(F32)
        pick = jnp.where(pos == place, 1.0, 0.0).astype(BF16)
        return jnp.dot(pick, x_ref[...], preferred_element_type=F32).astype(BF16)

    def gather_step(q, c):
        xbuf[q] = gather(q)

        @pl.when(q >= 2)
        def _():
            x_copy(q - 1).start()
        return c
    lax.fori_loop(1, n, gather_step, 0)
    hbuf[0] = gather(0)
    x_copy(n - 1).start()

    @pl.when(me != 0)
    def _():
        s1_copy(me).wait_recv()

    def s2_send_step(k, c):
        s2_copy(k).start()
        return c
    lax.fori_loop(1, half, s2_send_step, 0)

    def swiglu(rows, weights):
        mid = jnp.dot(rows, weights[pl.ds(0, d_model), :], preferred_element_type=F32)
        a = mid[:, :d_ff]
        u = (a * jax.nn.sigmoid(a) * mid[:, d_ff:]).astype(BF16)
        return jnp.dot(u, weights[pl.ds(d_model, d_ff), :], preferred_element_type=F32).astype(BF16)

    def send_back(q):
        pl.semaphore_wait(free.at[q], 1)
        h_copy(q).start()

    def expert_step(q, c):
        @pl.when(q >= 1)
        def _():
            x_copy(q).wait()
            pl.semaphore_signal(free.at[q], inc=1, device_id={'ep': shifted(q, 1)}, device_id_type=MESH)
        hbuf[q] = swiglu(hbuf[q], own)

        @pl.when(q > LAG)
        def _():
            send_back(q - LAG)
        return c
    lax.fori_loop(0, n, expert_step, 0)
    for q in range(n - LAG, n):
        send_back(q)

    tile = 256
    tiles = tokens // tile
    own_lane = lax.broadcasted_iota(jnp.int32, (tile, lanes), 1)
    pos_lane = lax.broadcasted_iota(jnp.int32, (tile, cap_p), 1).astype(F32)

    def combine(e, rows):
        def body(i, c):
            at = pl.ds(pl.multiple_of(i * tile, tile), tile)
            mine = own_lane == e
            place = jnp.sum(jnp.where(mine, slot_t[at, :], 0.0), axis=1, keepdims=True)
            gate = jnp.sum(jnp.where(mine, gate_t[at, :], 0.0), axis=1, keepdims=True)
            pick = jnp.where(pos_lane == place, 1.0, 0.0).astype(BF16)
            acc[at, :] += gate * jnp.dot(pick, rows[...], preferred_element_type=F32)
            return c
        lax.fori_loop(0, tiles, body, 0)

    def hot_gate(i, c):
        at = pl.ds(pl.multiple_of(i * tile, tile), tile)
        tok = lax.broadcasted_iota(jnp.int32, (tile, hot_tok_ref.shape[1]), 0) + i * tile
        hot_w[at, :] = jnp.sum(jnp.where(hot_tok_ref[...] == tok, hot_g_ref[...], 0.0), axis=1, keepdims=True)
        acc[at, :] = jnp.zeros((tile, d_model), F32)
        return c
    lax.fori_loop(0, tiles, hot_gate, 0)
    combine(me, hbuf.at[0])

    def combine_step(q, c):
        @pl.when(q == HOT_STEP - 4)
        def _():
            def arrived(k, c):
                s2_arrival(k).wait_recv()
                s2_copy(k).wait_send()
                return c
            lax.fori_loop(1, half, arrived, 0)
            s3_copy(core).start()

        @pl.when(q == HOT_STEP)
        def _():
            s3_copy(core).wait_send()
            s3_copy(1 - core).wait_recv()

            def hot_step(i, c):
                at = pl.ds(pl.multiple_of(i * tile, tile), tile)
                acc[at, :] += hot_w[at, :] * swiglu(x_ref[at, :], hot).astype(F32)
                return c
            lax.fori_loop(0, tiles, hot_step, 0)

        h_copy(q).wait()
        combine(shifted(q, 1), xbuf.at[q])
        return c
    lax.fori_loop(1, n, combine_step, 0)

    @pl.when(me == 0)
    def _():
        def sent(d, c):
            s1_copy(d).wait_send()
            return c
        lax.fori_loop(1, n, sent, 0)

    def store(i, c):
        at = pl.ds(pl.multiple_of(i * tile, tile), tile)
        out_ref[at, :] = acc[at, :].astype(BF16)
        return c
    lax.fori_loop(0, tiles, store, 0)


def solution(mesh):
    n = mesh.shape['ep']
    row_spec = P(('dp', 'ep'), None)
    list_spec = P(('dp', 'ep'))
    expert_spec = P('ep', None, None)

    def local_layer(x, ids, gates, hot_tok, hot_g, wg, wu, wd):
        tokens, d_model = x.shape
        top_k = ids.shape[1]
        d_ff = wg.shape[2]
        cap = (tokens * top_k + n - 2) // (n - 1)
        cap_p = -(-cap // 16) * 16
        lanes = -(-n // 128) * 128
        half = n // 2
        vmem = pl.BlockSpec(memory_space=pltpu.VMEM)
        hbm = pl.BlockSpec(memory_space=pltpu.HBM)
        dma = pltpu.SemaphoreType.DMA
        return pl.pallas_call(
            functools.partial(moe_kernel, n, cap_p),
            out_shape=jax.ShapeDtypeStruct((tokens, d_model), BF16),
            in_specs=[vmem] * 5 + [hbm] * 3,
            out_specs=vmem,
            scratch_shapes=[
                pltpu.VMEM((d_model + d_ff, d_model), BF16),
                pltpu.VMEM((d_model + d_ff, d_model), BF16),
                pltpu.VMEM((n, cap_p, d_model), BF16),
                pltpu.VMEM((n, cap_p, d_model), BF16),
                pltpu.VMEM((tokens, lanes), F32),
                pltpu.VMEM((tokens, lanes), F32),
                pltpu.VMEM((lanes, tokens), F32),
                pltpu.VMEM((tokens, 1), F32),
                pltpu.VMEM((tokens, d_model), F32),
                dma((3,)), dma((n,)), dma, dma((half,)), dma((half,)), dma, dma,
                dma((n,)), dma((n,)), dma((n,)), dma((n,)),
                pltpu.SemaphoreType.REGULAR((n,)),
            ],
            compiler_params=pltpu.CompilerParams(
                collective_id=0, has_side_effects=True, vmem_limit_bytes=67_043_328),
        )(x, ids, gates, hot_tok.reshape(1, -1), hot_g.reshape(1, -1), wg, wu, wd)

    return jax.shard_map(local_layer, mesh=mesh,
                         in_specs=(row_spec, row_spec, row_spec, list_spec, list_spec, expert_spec, expert_spec, expert_spec),
                         out_specs=row_spec, check_vma=False)
```

```python
import functools

import jax
import jax.numpy as jnp
from jax import lax
from jax.experimental import pallas as pl
from jax.experimental.pallas import tpu as pltpu
from jax.sharding import PartitionSpec as P

MESH = pl.DeviceIdType.MESH
F32 = jnp.float32
BF16 = jnp.bfloat16
OFFSETS = ((0, 0), (1, 1), (3, 3), (1, 3), (3, 1), (2, 2), (1, 2), (3, 2), (2, 1), (2, 3),
           (1, 0), (3, 0), (0, 1), (0, 3), (2, 0), (0, 2))
SIDE = 4
RING = (0, 1, 3, 2)
ARRIVALS = tuple(sorted(OFFSETS, key=lambda o: max(RING.index(o[0]), RING.index(o[1]))))
EARLY = 16
HOT_SHARE = 18
HOT_RUN = 24


def packed(values):
    return sum(v << (2 * i) for i, v in enumerate(values))


def entry(table, i):
    return lax.rem(lax.shift_right_logical(jnp.int32(table), 2 * i), SIDE)


def place_of(order, t):
    j = lax.div(t, 2)
    i = lax.max(j - 1, 0)
    near = lax.min(j, 1)
    dx = entry(packed([o[0] for o in order[1:]]), i) * near
    dy = entry(packed([o[1] for o in order[1:]]), i) * near
    return dx, dy, lax.rem(t, 2)


def moe_kernel(n, cap_p, x_ref, ids_ref, gates_ref, hot_tok_ref, hot_g_ref, wg_ref, wu_ref, wd_ref, out_ref,
               own, hot, xbuf, hbuf, ring_x, ring_y, tab_x, tab_y, slot_t, gate_t, slot_r, slot_x, hot_w, acc,
               w_sem, s1_send, s1_recv, s2_send, s2_recv, s3_send, s3_recv,
               rows_send, rows_recv, tabs_send, tabs_recv, part_send, part_recv, h_send, h_recv, out_sem, free):
    tokens, d_model = x_ref.shape
    top_k = ids_ref.shape[0]
    d_ff = wg_ref.shape[2]
    lanes = slot_t.shape[1]
    chunk = own.shape[0] // n
    half = n // 2
    wide = d_model // 2
    me = lax.axis_index('ep')
    core = lax.rem(me, 2)
    chip = lax.div(me, 2)
    px = lax.rem(chip, SIDE)
    py = lax.div(chip, SIDE)

    def dev(dx, dy, dc):
        tx = lax.rem(px + dx + SIDE, SIDE)
        ty = lax.rem(py + dy + SIDE, SIDE)
        return (ty * SIDE + tx) * 2 + lax.rem(core + dc, 2)

    def slot_of(dx, dy, dc):
        return (dy * SIDE + dx) * 2 + dc

    def remote(src, dst, send, recv, device):
        return pltpu.make_async_remote_copy(src_ref=src, dst_ref=dst, send_sem=send, recv_sem=recv,
                                            device_id={'ep': device}, device_id_type=MESH)

    barrier = pltpu.get_barrier_semaphore()

    def greet(k, c):
        pl.semaphore_signal(barrier, inc=1, device_id={'ep': lax.rem(me + k, n)}, device_id_type=MESH)
        return c
    lax.fori_loop(1, n, greet, 0)

    w_copies = (
        pltpu.make_async_copy(wg_ref.at[0], own.at[pl.ds(0, d_model), pl.ds(0, d_ff)], w_sem.at[0]),
        pltpu.make_async_copy(wu_ref.at[0], own.at[pl.ds(0, d_model), pl.ds(d_ff, d_ff)], w_sem.at[1]),
        pltpu.make_async_copy(wd_ref.at[0], own.at[pl.ds(d_model, d_ff), :], w_sem.at[2]),
    )
    for copy in w_copies:
        copy.start()
    pl.semaphore_wait(barrier, n - 1)

    cols = (pl.ds(0, wide), pl.ds(wide, wide))
    rings = (ring_x, ring_y)
    tabs = (tab_x, tab_y)

    def step_of(axis, a):
        return dev(a, 0, 0) if axis == 0 else dev(0, a, 0)

    def rows_copy(axis, a):
        return remote(x_ref.at[:, cols[axis]], rings[axis].at[a - 1], rows_send.at[axis, a], rows_recv.at[axis, a],
                      step_of(axis, a))

    def tabs_copy(axis, a):
        if axis == 0:
            src = slot_x.at[pl.ds(pl.multiple_of(lax.rem(px + a, SIDE) * 8, 8), 8), :]
        else:
            src = slot_r.at[pl.ds(pl.multiple_of(lax.rem(py + a, SIDE) * 8, 8), 8), :]
        return remote(src, tabs[axis].at[a], tabs_send.at[axis, a], tabs_recv.at[axis, a], step_of(axis, a))

    for a in RING[1:]:
        for axis in (0, 1):
            rows_copy(axis, a).start()

    expert = lax.broadcasted_iota(jnp.int32, (lanes, tokens), 0)
    chosen = jnp.zeros((lanes, tokens), F32)
    gate_sum = jnp.zeros((lanes, tokens), F32)
    for j in range(top_k):
        hit = ids_ref[pl.ds(j, 1), :] == expert
        chosen = jnp.where(hit, 1.0, chosen)
        gate_sum = jnp.where(hit, gates_ref[pl.ds(j, 1), :], gate_sum)
    gate_t[...] = gate_sum.T
    chosen_b = chosen.astype(BF16)
    step = 256
    for r in range(tokens // step):
        upto = lax.broadcasted_iota(jnp.int32, (tokens, step), 1) + r * step
        before = jnp.where(lax.broadcasted_iota(jnp.int32, (tokens, step), 0) < upto, 1.0, 0.0).astype(BF16)
        rank = jnp.dot(chosen_b, before, preferred_element_type=F32)
        slot_r[:, pl.ds(r * step, step)] = jnp.where(chosen[:, r * step:(r + 1) * step] > 0.5, rank, -1.0)
    slot_t[...] = slot_r[...].T
    for tx in range(SIDE):
        for ty in range(SIDE):
            slot_x[pl.ds(tx * 8 + ty * 2, 2), :] = slot_r[pl.ds((ty * SIDE + tx) * 2, 2), :]
    tab_x[0] = slot_x[pl.ds(pl.multiple_of(px * 8, 8), 8), :]
    tab_y[0] = slot_r[pl.ds(pl.multiple_of(py * 8, 8), 8), :]
    for a in RING[1:]:
        for axis in (0, 1):
            tabs_copy(axis, a).start()

    def part(axis, a, m):
        b = entry(packed(RING[1:] + RING[:1]), lax.div(m, 2))
        dc = lax.rem(m, 2)
        q = slot_of(a, b, dc) if axis == 0 else slot_of(b, a, dc)
        target = dev(0, b, dc) if axis == 0 else dev(b, 0, dc)
        row = lax.rem((py if axis == 0 else px) + b, SIDE) * 2 + lax.rem(core + dc, 2)
        return q, target, row

    def part_copy(axis, q, target):
        return remote(xbuf.at[q, :, cols[axis]], hbuf.at[q, :, cols[axis]], part_send.at[axis, q],
                      part_recv.at[axis, q], target)

    pos = lax.broadcasted_iota(jnp.int32, (cap_p, tokens), 0).astype(F32)

    def gather(axis, a, m):
        q, target, row = part(axis, a, m)

        @pl.when(target != 0)
        def _():
            source = x_ref[:, cols[axis]] if a == 0 else rings[axis][a - 1]
            pick = jnp.where(pos == tabs[axis][a, pl.ds(row, 1), :], 1.0, 0.0).astype(BF16)
            xbuf[q, :, cols[axis]] = jnp.dot(pick, source, preferred_element_type=F32).astype(BF16)

    def post(axis, a, m):
        q, target, row = part(axis, a, m)

        @pl.when((target != 0) & (target != me))
        def _():
            part_copy(axis, q, target).start()

        @pl.when((target != 0) & (target == me))
        def _():
            hbuf[q, :, cols[axis]] = xbuf[q, :, cols[axis]]

    for a in RING:
        if a:
            for axis in (0, 1):
                rows_copy(axis, a).wait_recv()
                tabs_copy(axis, a).wait_recv()

        def gather_step(m, c, a=a):
            gather(0, a, m)

            @pl.when(m > 0)
            def _():
                post(1, a, m - 1)
            gather(1, a, m)
            post(0, a, m)
            return c
        lax.fori_loop(0, 2 * SIDE, gather_step, 0)
        post(1, a, jnp.int32(2 * SIDE - 1))

    for a in RING[1:]:
        for axis in (0, 1):
            rows_copy(axis, a).wait_send()
            tabs_copy(axis, a).wait_send()
    for copy in w_copies:
        copy.wait()

    def swiglu(rows, weights):
        mid = jnp.dot(rows, weights[pl.ds(0, d_model), :], preferred_element_type=F32)
        a = mid[:, :d_ff]
        u = (a * jax.nn.sigmoid(a) * mid[:, d_ff:]).astype(BF16)
        return jnp.dot(u, weights[pl.ds(d_model, d_ff), :], preferred_element_type=F32).astype(BF16)

    def h_copy(dx, dy, dc):
        q = slot_of(dx, dy, dc)
        return remote(hbuf.at[q], xbuf.at[q], h_send.at[q], h_recv.at[q], dev(-dx, -dy, dc))

    def expert_step(t, c):
        dx, dy, dc = place_of(ARRIVALS, t)
        q = slot_of(dx, dy, dc)
        for axis, target in ((0, dev(0, dy, dc)), (1, dev(dx, 0, dc))):
            @pl.when((target != 0) & (target != me))
            def _():
                part_copy(axis, q, target).wait_send()
        maker = dev(dx, dy, dc)

        @pl.when((maker != 0) & (maker != me))
        def _():
            pl.semaphore_signal(free.at[q], inc=1, device_id={'ep': maker}, device_id_type=MESH)

        @pl.when(me != 0)
        def _():
            for axis, target in ((0, dev(0, dy, dc)), (1, dev(dx, 0, dc))):
                @pl.when(target != me)
                def _():
                    part_copy(axis, q, target).wait_recv()
            hbuf[q] = swiglu(hbuf[q], own)
        return c
    lax.fori_loop(0, n, expert_step, 0)

    def piece(d):
        return pl.ds(pl.multiple_of((lax.rem(d, 2) * half + lax.div(d, 2)) * chunk, chunk), chunk)

    def s1_copy(d):
        return remote(own.at[piece(d), :], hot.at[piece(d), :], s1_send.at[d], s1_recv, d)

    def s2_copy(j, sign=1):
        dx, dy, dc = place_of(OFFSETS, 2 * j)
        peer = dev(sign * dx, sign * dy, 0)
        held = piece(me if sign == 1 else peer)
        return remote(hot.at[held, :], hot.at[held, :], s2_send.at[j], s2_recv.at[j], peer)

    def core_half(c):
        return hot.at[pl.ds(pl.multiple_of(c * half * chunk, chunk), half * chunk), :]

    def s3_copy(c):
        return remote(core_half(c), core_half(c), s3_send, s3_recv, dev(0, 0, 1))

    @pl.when(me == 0)
    def _():
        hot[pl.ds(0, chunk), :] = own[pl.ds(0, chunk), :]

        def send(t, c):
            dx, dy, dc = place_of(OFFSETS, t)
            s1_copy(dev(dx, dy, dc)).start()
            return c
        lax.fori_loop(1, n, send, 0)

    def send_back(t, c):
        dx, dy, dc = place_of(OFFSETS, t)

        @pl.when(me != 0)
        def _():
            pl.semaphore_wait(free.at[slot_of(dx, dy, dc)], 1)
            h_copy(dx, dy, dc).start()
        return c
    lax.fori_loop(1, EARLY, send_back, 0)

    @pl.when(me != 0)
    def _():
        s1_copy(me).wait_recv()

    def s2_step(j, c):
        s2_copy(j).start()
        return c
    lax.fori_loop(1, half, s2_step, 0)
    lax.fori_loop(EARLY, n, send_back, 0)

    tile = 256
    tiles = tokens // tile
    own_lane = lax.broadcasted_iota(jnp.int32, (tile, lanes), 1)
    pos_lane = lax.broadcasted_iota(jnp.int32, (tile, cap_p), 1).astype(F32)

    def combine(e, rows):
        def body(i, c):
            at = pl.ds(pl.multiple_of(i * tile, tile), tile)
            mine = own_lane == e
            place = jnp.sum(jnp.where(mine, slot_t[at, :], 0.0), axis=1, keepdims=True)
            gate = jnp.sum(jnp.where(mine, gate_t[at, :], 0.0), axis=1, keepdims=True)
            pick = jnp.where(pos_lane == place, 1.0, 0.0).astype(BF16)
            acc[at, :] += gate * jnp.dot(pick, rows[...], preferred_element_type=F32)
            return c
        lax.fori_loop(0, tiles, body, 0)

    def hot_gate(i, c):
        at = pl.ds(pl.multiple_of(i * tile, tile), tile)
        tok = lax.broadcasted_iota(jnp.int32, (tile, hot_tok_ref.shape[1]), 0) + i * tile
        hot_w[at, :] = jnp.sum(jnp.where(hot_tok_ref[...] == tok, hot_g_ref[...], 0.0), axis=1, keepdims=True)
        acc[at, :] = jnp.zeros((tile, d_model), F32)
        return c
    lax.fori_loop(0, tiles, hot_gate, 0)

    @pl.when(me != 0)
    def _():
        combine(me, hbuf.at[0])

    def combine_step(t, c):
        @pl.when(t == HOT_SHARE)
        def _():
            def arrived(j, c):
                s2_copy(j, -1).wait_recv()
                s2_copy(j).wait_send()
                return c
            lax.fori_loop(1, half, arrived, 0)
            s3_copy(core).start()

        @pl.when(t == HOT_RUN)
        def _():
            s3_copy(core).wait_send()
            s3_copy(1 - core).wait_recv()

            def hot_step(i, c):
                at = pl.ds(pl.multiple_of(i * tile, tile), tile)
                acc[at, :] += hot_w[at, :] * swiglu(x_ref[at, :], hot).astype(F32)
                return c
            lax.fori_loop(0, tiles, hot_step, 0)

        dx, dy, dc = place_of(OFFSETS, t)
        maker = dev(dx, dy, dc)

        @pl.when(me != 0)
        def _():
            h_copy(dx, dy, dc).wait_send()

        @pl.when(maker != 0)
        def _():
            h_copy(dx, dy, dc).wait_recv()
            combine(maker, xbuf.at[slot_of(dx, dy, dc)])
        return c
    lax.fori_loop(1, n, combine_step, 0)

    @pl.when(me == 0)
    def _():
        def sent(d, c):
            s1_copy(d).wait_send()
            return c
        lax.fori_loop(1, n, sent, 0)

    def out_copy(axis, i):
        at = pl.ds(pl.multiple_of(i * tile, tile), tile)
        return pltpu.make_async_copy(rings[axis].at[0, at, :], out_ref.at[at, cols[axis]], out_sem.at[axis, i])

    for i in range(tiles):
        for axis in (0, 1):
            rings[axis][0, pl.ds(i * tile, tile), :] = acc[pl.ds(i * tile, tile), cols[axis]].astype(BF16)
            if i:
                out_copy(axis, i - 1).start()
    for axis in (0, 1):
        out_copy(axis, tiles - 1).start()
    for i in range(tiles):
        for axis in (0, 1):
            out_copy(axis, i).wait()


def solution(mesh):
    n = mesh.shape['ep']
    row_spec = P(('dp', 'ep'), None)
    list_spec = P(('dp', 'ep'))
    expert_spec = P('ep', None, None)

    def local_layer(x, ids, gates, hot_tok, hot_g, wg, wu, wd):
        tokens, d_model = x.shape
        top_k = ids.shape[1]
        d_ff = wg.shape[2]
        cap = (tokens * top_k + n - 2) // (n - 1)
        cap_p = -(-cap // 16) * 16
        lanes = -(-n // 128) * 128
        half = n // 2
        vmem = pl.BlockSpec(memory_space=pltpu.VMEM)
        hbm = pl.BlockSpec(memory_space=pltpu.HBM)
        dma = pltpu.SemaphoreType.DMA
        return pl.pallas_call(
            functools.partial(moe_kernel, n, cap_p),
            out_shape=jax.ShapeDtypeStruct((tokens, d_model), BF16),
            in_specs=[vmem] * 5 + [hbm] * 3,
            out_specs=hbm,
            scratch_shapes=[
                pltpu.VMEM((d_model + d_ff, d_model), BF16),
                pltpu.VMEM((d_model + d_ff, d_model), BF16),
                pltpu.VMEM((n, cap_p, d_model), BF16),
                pltpu.VMEM((n, cap_p, d_model), BF16),
                pltpu.VMEM((SIDE - 1, tokens, d_model // 2), BF16),
                pltpu.VMEM((SIDE - 1, tokens, d_model // 2), BF16),
                pltpu.VMEM((SIDE, 2 * SIDE, tokens), F32),
                pltpu.VMEM((SIDE, 2 * SIDE, tokens), F32),
                pltpu.VMEM((tokens, lanes), F32),
                pltpu.VMEM((tokens, lanes), F32),
                pltpu.VMEM((lanes, tokens), F32),
                pltpu.VMEM((n, tokens), F32),
                pltpu.VMEM((tokens, 1), F32),
                pltpu.VMEM((tokens, d_model), F32),
                dma((3,)), dma((n,)), dma, dma((half,)), dma((half,)), dma, dma,
                dma((2, SIDE)), dma((2, SIDE)), dma((2, SIDE)), dma((2, SIDE)),
                dma((2, n)), dma((2, n)), dma((n,)), dma((n,)), dma((2, tokens // 256)),
                pltpu.SemaphoreType.REGULAR((n,)),
            ],
            compiler_params=pltpu.CompilerParams(
                collective_id=0, has_side_effects=True, vmem_limit_bytes=67_043_328),
        )(x, ids.T, gates.T, hot_tok.reshape(1, -1), hot_g.reshape(1, -1), wg, wu, wd)

    return jax.shard_map(local_layer, mesh=mesh,
                         in_specs=(row_spec, row_spec, row_spec, list_spec, list_spec, expert_spec, expert_spec, expert_spec),
                         out_specs=row_spec, check_vma=False)
```

```python
import functools

import jax
import jax.numpy as jnp
from jax import lax
from jax.experimental import pallas as pl
from jax.experimental.pallas import tpu as pltpu
from jax.sharding import PartitionSpec as P

MESH = pl.DeviceIdType.MESH
F32 = jnp.float32
BF16 = jnp.bfloat16
OFFSETS = ((0, 0), (1, 1), (3, 3), (1, 3), (3, 1), (2, 2), (1, 2), (3, 2), (2, 1), (2, 3),
           (1, 0), (3, 0), (0, 1), (0, 3), (2, 0), (0, 2))
SIDE = 4
RING = (0, 1, 3, 2)
ARRIVALS = tuple(sorted(OFFSETS, key=lambda o: max(RING.index(o[0]), RING.index(o[1]))))
HOT_LEG = 12
HOT_SHARE = 10
HOT_RUN = 16


def packed(values):
    return sum(v << (2 * i) for i, v in enumerate(values))


def entry(table, i):
    return lax.rem(lax.shift_right_logical(jnp.int32(table), 2 * i), SIDE)


def place_of(order, t):
    j = lax.div(t, 2)
    i = lax.max(j - 1, 0)
    near = lax.min(j, 1)
    dx = entry(packed([o[0] for o in order[1:]]), i) * near
    dy = entry(packed([o[1] for o in order[1:]]), i) * near
    return dx, dy, lax.rem(t, 2)


def moe_kernel(n, cap_p, x_ref, ids_ref, gates_ref, hot_tok_ref, hot_g_ref, wg_ref, wu_ref, wd_ref, out_ref,
               own, hot, xbuf, hbuf, ring_x, ring_y, tab_x, tab_y, slot_t, gate_t, slot_r, slot_x, hot_w, acc,
               w_sem, s1_send, s1_recv, s2_send, s2_recv, s3_send, s3_recv,
               rows_send, rows_recv, tabs_send, tabs_recv, part_send, part_recv, h1_send, h1_recv, h2_send, h2_recv, out_sem, free, ready):
    tokens, d_model = x_ref.shape
    top_k = ids_ref.shape[0]
    d_ff = wg_ref.shape[2]
    lanes = slot_t.shape[1]
    chunk = own.shape[0] // n
    half = n // 2
    wide = d_model // 2
    me = lax.axis_index('ep')
    core = lax.rem(me, 2)
    chip = lax.div(me, 2)
    px = lax.rem(chip, SIDE)
    py = lax.div(chip, SIDE)

    def dev(dx, dy, dc):
        tx = lax.rem(px + dx + SIDE, SIDE)
        ty = lax.rem(py + dy + SIDE, SIDE)
        return (ty * SIDE + tx) * 2 + lax.rem(core + dc, 2)

    def slot_of(dx, dy, dc):
        return (dy * SIDE + dx) * 2 + dc

    def remote(src, dst, send, recv, device):
        return pltpu.make_async_remote_copy(src_ref=src, dst_ref=dst, send_sem=send, recv_sem=recv,
                                            device_id={'ep': device}, device_id_type=MESH)

    barrier = pltpu.get_barrier_semaphore()

    def greet(k, c):
        pl.semaphore_signal(barrier, inc=1, device_id={'ep': lax.rem(me + k, n)}, device_id_type=MESH)
        return c
    lax.fori_loop(1, n, greet, 0)

    w_copies = (
        pltpu.make_async_copy(wg_ref.at[0], own.at[pl.ds(0, d_model), pl.ds(0, d_ff)], w_sem.at[0]),
        pltpu.make_async_copy(wu_ref.at[0], own.at[pl.ds(0, d_model), pl.ds(d_ff, d_ff)], w_sem.at[1]),
        pltpu.make_async_copy(wd_ref.at[0], own.at[pl.ds(d_model, d_ff), :], w_sem.at[2]),
    )
    for copy in w_copies:
        copy.start()
    pl.semaphore_wait(barrier, n - 1)

    cols = (pl.ds(0, wide), pl.ds(wide, wide))
    rings = (ring_x, ring_y)
    tabs = (tab_x, tab_y)

    def step_of(axis, a):
        return dev(a, 0, 0) if axis == 0 else dev(0, a, 0)

    def rows_copy(axis, a):
        return remote(x_ref.at[:, cols[axis]], rings[axis].at[a - 1], rows_send.at[axis, a], rows_recv.at[axis, a],
                      step_of(axis, a))

    def tabs_copy(axis, a):
        if axis == 0:
            src = slot_x.at[pl.ds(pl.multiple_of(lax.rem(px + a, SIDE) * 8, 8), 8), :]
        else:
            src = slot_r.at[pl.ds(pl.multiple_of(lax.rem(py + a, SIDE) * 8, 8), 8), :]
        return remote(src, tabs[axis].at[a], tabs_send.at[axis, a], tabs_recv.at[axis, a], step_of(axis, a))

    for a in RING[1:]:
        for axis in (0, 1):
            rows_copy(axis, a).start()

    expert = lax.broadcasted_iota(jnp.int32, (lanes, tokens), 0)
    chosen = jnp.zeros((lanes, tokens), F32)
    gate_sum = jnp.zeros((lanes, tokens), F32)
    for j in range(top_k):
        hit = ids_ref[pl.ds(j, 1), :] == expert
        chosen = jnp.where(hit, 1.0, chosen)
        gate_sum = jnp.where(hit, gates_ref[pl.ds(j, 1), :], gate_sum)
    gate_t[...] = gate_sum.T
    chosen_b = chosen.astype(BF16)
    step = 256
    for r in range(tokens // step):
        upto = lax.broadcasted_iota(jnp.int32, (tokens, step), 1) + r * step
        before = jnp.where(lax.broadcasted_iota(jnp.int32, (tokens, step), 0) < upto, 1.0, 0.0).astype(BF16)
        rank = jnp.dot(chosen_b, before, preferred_element_type=F32)
        slot_r[:, pl.ds(r * step, step)] = jnp.where(chosen[:, r * step:(r + 1) * step] > 0.5, rank, -1.0)
    slot_t[...] = slot_r[...].T
    for tx in range(SIDE):
        for ty in range(SIDE):
            slot_x[pl.ds(tx * 8 + ty * 2, 2), :] = slot_r[pl.ds((ty * SIDE + tx) * 2, 2), :]
    tab_x[0] = slot_x[pl.ds(pl.multiple_of(px * 8, 8), 8), :]
    tab_y[0] = slot_r[pl.ds(pl.multiple_of(py * 8, 8), 8), :]
    for a in RING[1:]:
        for axis in (0, 1):
            tabs_copy(axis, a).start()

    def part(axis, a, m):
        b = entry(packed(RING[1:] + RING[:1]), lax.div(m, 2))
        dc = lax.rem(m, 2)
        q = slot_of(a, b, dc) if axis == 0 else slot_of(b, a, dc)
        target = dev(0, b, dc) if axis == 0 else dev(b, 0, dc)
        row = lax.rem((py if axis == 0 else px) + b, SIDE) * 2 + lax.rem(core + dc, 2)
        return q, target, row

    def part_copy(axis, q, target):
        return remote(xbuf.at[q, :, cols[axis]], hbuf.at[q, :, cols[axis]], part_send.at[axis, q],
                      part_recv.at[axis, q], target)

    pos = lax.broadcasted_iota(jnp.int32, (cap_p, tokens), 0).astype(F32)

    def gather(axis, a, m):
        q, target, row = part(axis, a, m)

        @pl.when(target != 0)
        def _():
            source = x_ref[:, cols[axis]] if a == 0 else rings[axis][a - 1]
            pick = jnp.where(pos == tabs[axis][a, pl.ds(row, 1), :], 1.0, 0.0).astype(BF16)
            xbuf[q, :, cols[axis]] = jnp.dot(pick, source, preferred_element_type=F32).astype(BF16)

    def post(axis, a, m):
        q, target, row = part(axis, a, m)

        @pl.when((target != 0) & (target != me))
        def _():
            part_copy(axis, q, target).start()

        @pl.when((target != 0) & (target == me))
        def _():
            hbuf[q, :, cols[axis]] = xbuf[q, :, cols[axis]]

    for a in RING:
        if a:
            for axis in (0, 1):
                rows_copy(axis, a).wait_recv()
                tabs_copy(axis, a).wait_recv()

        def gather_step(m, c, a=a):
            gather(0, a, m)

            @pl.when(m > 0)
            def _():
                post(1, a, m - 1)
            gather(1, a, m)
            post(0, a, m)
            return c
        lax.fori_loop(0, 2 * SIDE, gather_step, 0)
        post(1, a, jnp.int32(2 * SIDE - 1))

    for a in RING[1:]:
        for axis in (0, 1):
            rows_copy(axis, a).wait_send()
            tabs_copy(axis, a).wait_send()
    for copy in w_copies:
        copy.wait()

    def swiglu(rows, weights):
        mid = jnp.dot(rows, weights[pl.ds(0, d_model), :], preferred_element_type=F32)
        a = mid[:, :d_ff]
        u = (a * jax.nn.sigmoid(a) * mid[:, d_ff:]).astype(BF16)
        return jnp.dot(u, weights[pl.ds(d_model, d_ff), :], preferred_element_type=F32).astype(BF16)

    def back1(axis, dx, dy, dc):
        q = slot_of(dx, dy, dc)
        relay = dev(0, -dy, dc) if axis == 0 else dev(-dx, 0, dc)
        return relay, remote(hbuf.at[q, :, cols[axis]], xbuf.at[q, :, cols[axis]], h1_send.at[axis, q],
                             h1_recv.at[axis, q], relay)

    def back2(axis, dx, dy, dc):
        q = slot_of(dx, dy, dc)
        source = dev(-dx, 0, 0) if axis == 0 else dev(0, -dy, 0)
        return remote(xbuf.at[q, :, cols[axis]], hbuf.at[q, :, cols[axis]], h2_send.at[axis, q],
                      h2_recv.at[axis, q], source)

    def across(axis, dx, dy, dc):
        return (dev(0, dy, dc), dx) if axis == 0 else (dev(dx, 0, dc), dy)

    def send_back(t):
        dx, dy, dc = place_of(ARRIVALS, t)
        q = slot_of(dx, dy, dc)
        for axis in (0, 1):
            relay, copy = back1(axis, dx, dy, dc)

            @pl.when((me != 0) & (relay != me))
            def _():
                pl.semaphore_wait(free.at[axis, q], 1)
                copy.start()

            @pl.when((me != 0) & (relay == me))
            def _():
                xbuf[q, :, cols[axis]] = hbuf[q, :, cols[axis]]

    def expert_step(t, c):
        dx, dy, dc = place_of(ARRIVALS, t)
        q = slot_of(dx, dy, dc)
        for axis in (0, 1):
            target, _ = across(axis, dx, dy, dc)

            @pl.when((target != 0) & (target != me))
            def _():
                part_copy(axis, q, target).wait_send()
                pl.semaphore_signal(free.at[axis, q], inc=1, device_id={'ep': target}, device_id_type=MESH)

        @pl.when(me != 0)
        def _():
            for axis in (0, 1):
                target, _ = across(axis, dx, dy, dc)

                @pl.when(target != me)
                def _():
                    part_copy(axis, q, target).wait_recv()
            hbuf[q] = swiglu(hbuf[q], own)

        @pl.when(t > 1)
        def _():
            send_back(t - 1)
        return c

    def piece(d):
        return pl.ds(pl.multiple_of((lax.rem(d, 2) * half + lax.div(d, 2)) * chunk, chunk), chunk)

    def s1_copy(d):
        return remote(own.at[piece(d), :], hot.at[piece(d), :], s1_send.at[d], s1_recv, d)

    def s2_copy(axis, a, b, arriving=False):
        first = a is None
        if first:
            peer = step_of(axis, -b if arriving else b)
            held = piece(peer if arriving else me)
            i = b - 1
        else:
            back = b if arriving else 0
            held = piece(dev(-a, -back, 0) if axis == 0 else dev(-back, -a, 0))
            peer = step_of(1 - axis, -b if arriving else b)
            i = SIDE - 1 + a * (SIDE - 1) + b - 1
        at = hot.at[held, cols[axis]]
        return remote(at, at, s2_send.at[axis, i], s2_recv.at[axis, i], peer)

    LEG1 = [(axis, None, b) for b in RING[1:] for axis in (0, 1)]
    LEG2 = [(axis, a, b) for a in RING for b in RING[1:] for axis in (0, 1)]

    def core_half(c):
        return hot.at[pl.ds(pl.multiple_of(c * half * chunk, chunk), half * chunk), :]

    def s3_copy(c):
        return remote(core_half(c), core_half(c), s3_send, s3_recv, dev(0, 0, 1))

    @pl.when(me == 0)
    def _():
        hot[pl.ds(0, chunk), :] = own[pl.ds(0, chunk), :]

        def send(t, c):
            dx, dy, dc = place_of(OFFSETS, t)
            s1_copy(dev(dx, dy, dc)).start()
            return c
        lax.fori_loop(1, n, send, 0)

    lax.fori_loop(0, n, expert_step, 0)
    send_back(jnp.int32(n - 1))

    @pl.when(me != 0)
    def _():
        s1_copy(me).wait_recv()
    for leg in LEG1:
        s2_copy(*leg).start()

    def forward(t):
        dx, dy, dc = place_of(ARRIVALS, t)
        q = slot_of(dx, dy, dc)
        for axis in (0, 1):
            maker, steps = across(axis, dx, dy, dc)

            @pl.when((maker != 0) & (maker != me))
            def _():
                back1(axis, dx, dy, dc)[1].wait_recv()

            @pl.when((maker != 0) & (steps != 0))
            def _():
                pl.semaphore_wait(ready.at[axis, q], 1)
                back2(axis, dx, dy, dc).start()

    def relay_step(t, c):
        @pl.when(t == HOT_LEG)
        def _():
            for leg in LEG1:
                s2_copy(*leg, arriving=True).wait_recv()
            for leg in LEG2:
                s2_copy(*leg).start()

        dx, dy, dc = place_of(ARRIVALS, t)
        q = slot_of(dx, dy, dc)
        for axis in (0, 1):
            relay, copy = back1(axis, dx, dy, dc)

            @pl.when((me != 0) & (relay != me))
            def _():
                copy.wait_send()
            _, steps = across(axis, dx, dy, dc)
            via = dev(dx, 0, 0) if axis == 0 else dev(0, dy, 0)

            @pl.when((steps != 0) & (dev(dx, dy, dc) != 0))
            def _():
                pl.semaphore_signal(ready.at[axis, q], inc=1, device_id={'ep': via}, device_id_type=MESH)

        @pl.when(t > 1)
        def _():
            forward(t - 1)
        return c
    lax.fori_loop(1, n, relay_step, 0)
    forward(jnp.int32(n - 1))

    tile = 256
    tiles = tokens // tile
    own_lane = lax.broadcasted_iota(jnp.int32, (tile, lanes), 1)
    pos_lane = lax.broadcasted_iota(jnp.int32, (tile, cap_p), 1).astype(F32)

    def combine(e, rows):
        def body(i, c):
            at = pl.ds(pl.multiple_of(i * tile, tile), tile)
            mine = own_lane == e
            place = jnp.sum(jnp.where(mine, slot_t[at, :], 0.0), axis=1, keepdims=True)
            gate = jnp.sum(jnp.where(mine, gate_t[at, :], 0.0), axis=1, keepdims=True)
            pick = jnp.where(pos_lane == place, 1.0, 0.0).astype(BF16)
            acc[at, :] += gate * jnp.dot(pick, rows[...], preferred_element_type=F32)
            return c
        lax.fori_loop(0, tiles, body, 0)

    def hot_gate(i, c):
        at = pl.ds(pl.multiple_of(i * tile, tile), tile)
        tok = lax.broadcasted_iota(jnp.int32, (tile, hot_tok_ref.shape[1]), 0) + i * tile
        hot_w[at, :] = jnp.sum(jnp.where(hot_tok_ref[...] == tok, hot_g_ref[...], 0.0), axis=1, keepdims=True)
        acc[at, :] = jnp.zeros((tile, d_model), F32)
        return c
    lax.fori_loop(0, tiles, hot_gate, 0)

    @pl.when(me != 0)
    def _():
        combine(me, hbuf.at[0])

    def combine_step(t, c):
        @pl.when(t == HOT_SHARE)
        def _():
            for leg in LEG2:
                s2_copy(*leg, arriving=True).wait_recv()
            for leg in LEG1 + LEG2:
                s2_copy(*leg).wait_send()
            s3_copy(core).start()

        @pl.when(t == HOT_RUN)
        def _():
            s3_copy(core).wait_send()
            s3_copy(1 - core).wait_recv()

            def hot_step(i, c):
                at = pl.ds(pl.multiple_of(i * tile, tile), tile)
                acc[at, :] += hot_w[at, :] * swiglu(x_ref[at, :], hot).astype(F32)
                return c
            lax.fori_loop(0, tiles, hot_step, 0)

        dx, dy, dc = place_of(ARRIVALS, t)
        q = slot_of(dx, dy, dc)
        for axis in (0, 1):
            through, steps = across(axis, dx, dy, dc)

            @pl.when((through != 0) & (steps != 0))
            def _():
                back2(axis, dx, dy, dc).wait_send()
        maker = dev(dx, dy, dc)

        @pl.when(maker != 0)
        def _():
            for axis in (0, 1):
                _, steps = across(axis, dx, dy, dc)

                @pl.when(steps != 0)
                def _():
                    back2(axis, dx, dy, dc).wait_recv()

                @pl.when(steps == 0)
                def _():
                    hbuf[q, :, cols[axis]] = xbuf[q, :, cols[axis]]
            combine(maker, hbuf.at[q])
        return c
    lax.fori_loop(1, n, combine_step, 0)

    @pl.when(me == 0)
    def _():
        def sent(d, c):
            s1_copy(d).wait_send()
            return c
        lax.fori_loop(1, n, sent, 0)

    def out_copy(axis, i):
        at = pl.ds(pl.multiple_of(i * tile, tile), tile)
        return pltpu.make_async_copy(rings[axis].at[0, at, :], out_ref.at[at, cols[axis]], out_sem.at[axis, i])

    for i in range(tiles):
        for axis in (0, 1):
            rings[axis][0, pl.ds(i * tile, tile), :] = acc[pl.ds(i * tile, tile), cols[axis]].astype(BF16)
            if i:
                out_copy(axis, i - 1).start()
    for axis in (0, 1):
        out_copy(axis, tiles - 1).start()
    for i in range(tiles):
        for axis in (0, 1):
            out_copy(axis, i).wait()


def solution(mesh):
    n = mesh.shape['ep']
    row_spec = P(('dp', 'ep'), None)
    list_spec = P(('dp', 'ep'))
    expert_spec = P('ep', None, None)

    def local_layer(x, ids, gates, hot_tok, hot_g, wg, wu, wd):
        tokens, d_model = x.shape
        top_k = ids.shape[1]
        d_ff = wg.shape[2]
        cap = (tokens * top_k + n - 2) // (n - 1)
        cap_p = -(-cap // 16) * 16
        lanes = -(-n // 128) * 128
        half = n // 2
        vmem = pl.BlockSpec(memory_space=pltpu.VMEM)
        hbm = pl.BlockSpec(memory_space=pltpu.HBM)
        dma = pltpu.SemaphoreType.DMA
        return pl.pallas_call(
            functools.partial(moe_kernel, n, cap_p),
            out_shape=jax.ShapeDtypeStruct((tokens, d_model), BF16),
            in_specs=[vmem] * 5 + [hbm] * 3,
            out_specs=hbm,
            scratch_shapes=[
                pltpu.VMEM((d_model + d_ff, d_model), BF16),
                pltpu.VMEM((d_model + d_ff, d_model), BF16),
                pltpu.VMEM((n, cap_p, d_model), BF16),
                pltpu.VMEM((n, cap_p, d_model), BF16),
                pltpu.VMEM((SIDE - 1, tokens, d_model // 2), BF16),
                pltpu.VMEM((SIDE - 1, tokens, d_model // 2), BF16),
                pltpu.VMEM((SIDE, 2 * SIDE, tokens), F32),
                pltpu.VMEM((SIDE, 2 * SIDE, tokens), F32),
                pltpu.VMEM((tokens, lanes), F32),
                pltpu.VMEM((tokens, lanes), F32),
                pltpu.VMEM((lanes, tokens), F32),
                pltpu.VMEM((n, tokens), F32),
                pltpu.VMEM((tokens, 1), F32),
                pltpu.VMEM((tokens, d_model), F32),
                dma((3,)), dma((n,)), dma, dma((2, half - 1)), dma((2, half - 1)), dma, dma,
                dma((2, SIDE)), dma((2, SIDE)), dma((2, SIDE)), dma((2, SIDE)),
                dma((2, n)), dma((2, n)), dma((2, n)), dma((2, n)), dma((2, n)), dma((2, n)), dma((2, tokens // 256)),
                pltpu.SemaphoreType.REGULAR((2, n)), pltpu.SemaphoreType.REGULAR((2, n)),
            ],
            compiler_params=pltpu.CompilerParams(
                collective_id=0, has_side_effects=True, vmem_limit_bytes=67_043_328),
        )(x, ids.T, gates.T, hot_tok.reshape(1, -1), hot_g.reshape(1, -1), wg, wu, wd)

    return jax.shard_map(local_layer, mesh=mesh,
                         in_specs=(row_spec, row_spec, row_spec, list_spec, list_spec, expert_spec, expert_spec, expert_spec),
                         out_specs=row_spec, check_vma=False)
```

```python
import functools

import jax
import jax.numpy as jnp
from jax import lax
from jax.experimental import pallas as pl
from jax.experimental.pallas import tpu as pltpu
from jax.sharding import PartitionSpec as P

MESH = pl.DeviceIdType.MESH
F32 = jnp.float32
BF16 = jnp.bfloat16
OFFSETS = ((0, 0), (1, 1), (3, 3), (1, 3), (3, 1), (2, 2), (1, 2), (3, 2), (2, 1), (2, 3),
           (1, 0), (3, 0), (0, 1), (0, 3), (2, 0), (0, 2))
SIDE = 4
RING = (0, 1, 3, 2)
ARRIVALS = ((0, 0), (1, 0), (0, 1), (3, 0), (0, 3), (1, 1), (2, 0), (0, 2), (1, 3), (3, 1), (3, 3), (2, 1), (1, 2), (2, 3), (3, 2), (2, 2))
HOT_LEG = 12
HOT_SHARE = 10
HOT_RUN = 16


def packed(values):
    return sum(v << (2 * i) for i, v in enumerate(values))


def entry(table, i):
    return lax.rem(lax.shift_right_logical(jnp.int32(table), 2 * i), SIDE)


def place_of(order, t):
    j = lax.div(t, 2)
    i = lax.max(j - 1, 0)
    near = lax.min(j, 1)
    dx = entry(packed([o[0] for o in order[1:]]), i) * near
    dy = entry(packed([o[1] for o in order[1:]]), i) * near
    return dx, dy, lax.rem(t, 2)


def moe_kernel(n, cap_p, x_ref, ids_ref, gates_ref, hot_tok_ref, hot_g_ref, wg_ref, wu_ref, wd_ref, out_ref,
               own, hot, xbuf, hbuf, ring_x, ring_y, tab_x, tab_y, slot_t, gate_t, slot_r, slot_x, hot_w, acc,
               w_sem, s1_send, s1_recv, s2_send, s2_recv, s3_send, s3_recv,
               rows_send, rows_recv, tabs_send, tabs_recv, part_send, part_recv, h1_send, h1_recv, h2_send, h2_recv, out_sem, free, ready):
    tokens, d_model = x_ref.shape
    top_k = ids_ref.shape[0]
    d_ff = wg_ref.shape[2]
    lanes = slot_t.shape[1]
    chunk = own.shape[0] // n
    half = n // 2
    wide = d_model // 2
    me = lax.axis_index('ep')
    core = lax.rem(me, 2)
    chip = lax.div(me, 2)
    px = lax.rem(chip, SIDE)
    py = lax.div(chip, SIDE)

    def dev(dx, dy, dc):
        tx = lax.rem(px + dx + SIDE, SIDE)
        ty = lax.rem(py + dy + SIDE, SIDE)
        return (ty * SIDE + tx) * 2 + lax.rem(core + dc, 2)

    def slot_of(dx, dy, dc):
        return (dy * SIDE + dx) * 2 + dc

    def remote(src, dst, send, recv, device):
        return pltpu.make_async_remote_copy(src_ref=src, dst_ref=dst, send_sem=send, recv_sem=recv,
                                            device_id={'ep': device}, device_id_type=MESH)

    barrier = pltpu.get_barrier_semaphore()

    def greet(k, c):
        pl.semaphore_signal(barrier, inc=1, device_id={'ep': lax.rem(me + k, n)}, device_id_type=MESH)
        return c
    lax.fori_loop(1, n, greet, 0)

    w_copies = (
        pltpu.make_async_copy(wg_ref.at[0], own.at[pl.ds(0, d_model), pl.ds(0, d_ff)], w_sem.at[0]),
        pltpu.make_async_copy(wu_ref.at[0], own.at[pl.ds(0, d_model), pl.ds(d_ff, d_ff)], w_sem.at[1]),
        pltpu.make_async_copy(wd_ref.at[0], own.at[pl.ds(d_model, d_ff), :], w_sem.at[2]),
    )
    for copy in w_copies:
        copy.start()
    pl.semaphore_wait(barrier, n - 1)

    cols = (pl.ds(0, wide), pl.ds(wide, wide))
    rings = (ring_x, ring_y)
    tabs = (tab_x, tab_y)

    def step_of(axis, a):
        return dev(a, 0, 0) if axis == 0 else dev(0, a, 0)

    def rows_copy(axis, a):
        return remote(x_ref.at[:, cols[axis]], rings[axis].at[a - 1], rows_send.at[axis, a], rows_recv.at[axis, a],
                      step_of(axis, a))

    def tabs_copy(axis, a):
        if axis == 0:
            src = slot_x.at[pl.ds(pl.multiple_of(lax.rem(px + a, SIDE) * 8, 8), 8), :]
        else:
            src = slot_r.at[pl.ds(pl.multiple_of(lax.rem(py + a, SIDE) * 8, 8), 8), :]
        return remote(src, tabs[axis].at[a], tabs_send.at[axis, a], tabs_recv.at[axis, a], step_of(axis, a))

    def rows_onward(axis, ahead):
        at = pl.ds(0 if ahead else tokens // 2, tokens // 2)
        ring = rings[axis]
        i = 2 if ahead else 0
        return remote(ring.at[0 if ahead else 2, at, :], ring.at[1, at, :], rows_send.at[axis, i],
                      rows_recv.at[axis, i], step_of(axis, 1 if ahead else -1))

    for a in (1, 3):
        for axis in (0, 1):
            rows_copy(axis, a).start()

    expert = lax.broadcasted_iota(jnp.int32, (lanes, tokens), 0)
    chosen = jnp.zeros((lanes, tokens), F32)
    gate_sum = jnp.zeros((lanes, tokens), F32)
    for j in range(top_k):
        hit = ids_ref[pl.ds(j, 1), :] == expert
        chosen = jnp.where(hit, 1.0, chosen)
        gate_sum = jnp.where(hit, gates_ref[pl.ds(j, 1), :], gate_sum)
    gate_t[...] = gate_sum.T
    chosen_b = chosen.astype(BF16)
    step = 256
    for r in range(tokens // step):
        upto = lax.broadcasted_iota(jnp.int32, (tokens, step), 1) + r * step
        before = jnp.where(lax.broadcasted_iota(jnp.int32, (tokens, step), 0) < upto, 1.0, 0.0).astype(BF16)
        rank = jnp.dot(chosen_b, before, preferred_element_type=F32)
        slot_r[:, pl.ds(r * step, step)] = jnp.where(chosen[:, r * step:(r + 1) * step] > 0.5, rank, -1.0)
    slot_t[...] = slot_r[...].T
    for tx in range(SIDE):
        for ty in range(SIDE):
            slot_x[pl.ds(tx * 8 + ty * 2, 2), :] = slot_r[pl.ds((ty * SIDE + tx) * 2, 2), :]
    tab_x[0] = slot_x[pl.ds(pl.multiple_of(px * 8, 8), 8), :]
    tab_y[0] = slot_r[pl.ds(pl.multiple_of(py * 8, 8), 8), :]
    for a in RING[1:]:
        for axis in (0, 1):
            tabs_copy(axis, a).start()

    def part(axis, a, m):
        b = entry(packed(RING[1:] + RING[:1]), lax.div(m, 2))
        dc = lax.rem(m, 2)
        q = slot_of(a, b, dc) if axis == 0 else slot_of(b, a, dc)
        target = dev(0, b, dc) if axis == 0 else dev(b, 0, dc)
        row = lax.rem((py if axis == 0 else px) + b, SIDE) * 2 + lax.rem(core + dc, 2)
        return q, target, row

    def part_copy(axis, q, target):
        return remote(xbuf.at[q, :, cols[axis]], hbuf.at[q, :, cols[axis]], part_send.at[axis, q],
                      part_recv.at[axis, q], target)

    pos = lax.broadcasted_iota(jnp.int32, (cap_p, tokens), 0).astype(F32)

    def gather(axis, a, m):
        q, target, row = part(axis, a, m)

        @pl.when(target != 0)
        def _():
            source = x_ref[:, cols[axis]] if a == 0 else rings[axis][a - 1]
            pick = jnp.where(pos == tabs[axis][a, pl.ds(row, 1), :], 1.0, 0.0).astype(BF16)
            xbuf[q, :, cols[axis]] = jnp.dot(pick, source, preferred_element_type=F32).astype(BF16)

    def post(axis, a, m):
        q, target, row = part(axis, a, m)

        @pl.when((target != 0) & (target != me))
        def _():
            part_copy(axis, q, target).start()

        @pl.when((target != 0) & (target == me))
        def _():
            hbuf[q, :, cols[axis]] = xbuf[q, :, cols[axis]]

    for a in RING:
        for axis in (0, 1):
            if a == 1:
                for b in (1, 3):
                    rows_copy(axis, b).wait_recv()
                    rows_onward(axis, b == 1).start()
            if a == 2:
                for ahead in (True, False):
                    rows_onward(axis, ahead).wait_recv()
            if a:
                tabs_copy(axis, a).wait_recv()

        def gather_step(m, c, a=a):
            gather(0, a, m)

            @pl.when(m > 0)
            def _():
                post(1, a, m - 1)
            gather(1, a, m)
            post(0, a, m)
            return c
        lax.fori_loop(0, 2 * SIDE, gather_step, 0)
        post(1, a, jnp.int32(2 * SIDE - 1))

    for axis in (0, 1):
        for a in (1, 3):
            rows_copy(axis, a).wait_send()
            rows_onward(axis, a == 1).wait_send()
        for a in RING[1:]:
            tabs_copy(axis, a).wait_send()
    for copy in w_copies:
        copy.wait()

    def swiglu(rows, weights):
        mid = jnp.dot(rows, weights[pl.ds(0, d_model), :], preferred_element_type=F32)
        a = mid[:, :d_ff]
        u = (a * jax.nn.sigmoid(a) * mid[:, d_ff:]).astype(BF16)
        return jnp.dot(u, weights[pl.ds(d_model, d_ff), :], preferred_element_type=F32).astype(BF16)

    def back1(axis, dx, dy, dc):
        q = slot_of(dx, dy, dc)
        relay = dev(0, -dy, dc) if axis == 0 else dev(-dx, 0, dc)
        return relay, remote(hbuf.at[q, :, cols[axis]], xbuf.at[q, :, cols[axis]], h1_send.at[axis, q],
                             h1_recv.at[axis, q], relay)

    def back2(axis, dx, dy, dc):
        q = slot_of(dx, dy, dc)
        source = dev(-dx, 0, 0) if axis == 0 else dev(0, -dy, 0)
        return remote(xbuf.at[q, :, cols[axis]], hbuf.at[q, :, cols[axis]], h2_send.at[axis, q],
                      h2_recv.at[axis, q], source)

    def across(axis, dx, dy, dc):
        return (dev(0, dy, dc), dx) if axis == 0 else (dev(dx, 0, dc), dy)

    def send_back(t):
        dx, dy, dc = place_of(ARRIVALS, t)
        q = slot_of(dx, dy, dc)
        for axis in (0, 1):
            relay, copy = back1(axis, dx, dy, dc)

            @pl.when((me != 0) & (relay != me))
            def _():
                pl.semaphore_wait(free.at[axis, q], 1)
                copy.start()

            @pl.when((me != 0) & (relay == me))
            def _():
                xbuf[q, :, cols[axis]] = hbuf[q, :, cols[axis]]

    def expert_step(t, c):
        dx, dy, dc = place_of(ARRIVALS, t)
        q = slot_of(dx, dy, dc)
        for axis in (0, 1):
            target, _ = across(axis, dx, dy, dc)

            @pl.when((target != 0) & (target != me))
            def _():
                part_copy(axis, q, target).wait_send()
                pl.semaphore_signal(free.at[axis, q], inc=1, device_id={'ep': target}, device_id_type=MESH)

        @pl.when(me != 0)
        def _():
            for axis in (0, 1):
                target, _ = across(axis, dx, dy, dc)

                @pl.when(target != me)
                def _():
                    part_copy(axis, q, target).wait_recv()
            hbuf[q] = swiglu(hbuf[q], own)

        @pl.when(t > 1)
        def _():
            send_back(t - 1)
        return c

    def piece(d):
        return pl.ds(pl.multiple_of((lax.rem(d, 2) * half + lax.div(d, 2)) * chunk, chunk), chunk)

    def s1_copy(d):
        return remote(own.at[piece(d), :], hot.at[piece(d), :], s1_send.at[d], s1_recv, d)

    def s2_copy(axis, a, b, arriving=False):
        first = a is None
        if first:
            peer = step_of(axis, -b if arriving else b)
            held = piece(peer if arriving else me)
            i = b - 1
        else:
            back = b if arriving else 0
            held = piece(dev(-a, -back, 0) if axis == 0 else dev(-back, -a, 0))
            peer = step_of(1 - axis, -b if arriving else b)
            i = SIDE - 1 + a * (SIDE - 1) + b - 1
        at = hot.at[held, cols[axis]]
        return remote(at, at, s2_send.at[axis, i], s2_recv.at[axis, i], peer)

    LEG1 = [(axis, None, b) for b in RING[1:] for axis in (0, 1)]
    LEG2 = [(axis, a, b) for a in RING for b in RING[1:] for axis in (0, 1)]

    def core_half(c):
        return hot.at[pl.ds(pl.multiple_of(c * half * chunk, chunk), half * chunk), :]

    def s3_copy(c):
        return remote(core_half(c), core_half(c), s3_send, s3_recv, dev(0, 0, 1))

    @pl.when(me == 0)
    def _():
        hot[pl.ds(0, chunk), :] = own[pl.ds(0, chunk), :]

        def send(t, c):
            dx, dy, dc = place_of(OFFSETS, t)
            s1_copy(dev(dx, dy, dc)).start()
            return c
        lax.fori_loop(1, n, send, 0)

    lax.fori_loop(0, n, expert_step, 0)
    send_back(jnp.int32(n - 1))

    @pl.when(me != 0)
    def _():
        s1_copy(me).wait_recv()
    for leg in LEG1:
        s2_copy(*leg).start()

    def forward(t):
        dx, dy, dc = place_of(ARRIVALS, t)
        q = slot_of(dx, dy, dc)
        for axis in (0, 1):
            maker, steps = across(axis, dx, dy, dc)

            @pl.when((maker != 0) & (maker != me))
            def _():
                back1(axis, dx, dy, dc)[1].wait_recv()

            @pl.when((maker != 0) & (steps != 0))
            def _():
                pl.semaphore_wait(ready.at[axis, q], 1)
                back2(axis, dx, dy, dc).start()

    def relay_step(t, c):
        @pl.when(t == HOT_LEG)
        def _():
            for leg in LEG1:
                s2_copy(*leg, arriving=True).wait_recv()
            for leg in LEG2:
                s2_copy(*leg).start()

        dx, dy, dc = place_of(ARRIVALS, t)
        q = slot_of(dx, dy, dc)
        for axis in (0, 1):
            relay, copy = back1(axis, dx, dy, dc)

            @pl.when((me != 0) & (relay != me))
            def _():
                copy.wait_send()
            _, steps = across(axis, dx, dy, dc)
            via = dev(dx, 0, 0) if axis == 0 else dev(0, dy, 0)

            @pl.when((steps != 0) & (dev(dx, dy, dc) != 0))
            def _():
                pl.semaphore_signal(ready.at[axis, q], inc=1, device_id={'ep': via}, device_id_type=MESH)

        @pl.when(t > 1)
        def _():
            forward(t - 1)
        return c
    lax.fori_loop(1, n, relay_step, 0)
    forward(jnp.int32(n - 1))

    tile = 256
    tiles = tokens // tile
    own_lane = lax.broadcasted_iota(jnp.int32, (tile, lanes), 1)
    pos_lane = lax.broadcasted_iota(jnp.int32, (tile, cap_p), 1).astype(F32)

    def combine(e, rows):
        def body(i, c):
            at = pl.ds(pl.multiple_of(i * tile, tile), tile)
            mine = own_lane == e
            place = jnp.sum(jnp.where(mine, slot_t[at, :], 0.0), axis=1, keepdims=True)
            gate = jnp.sum(jnp.where(mine, gate_t[at, :], 0.0), axis=1, keepdims=True)
            pick = jnp.where(pos_lane == place, 1.0, 0.0).astype(BF16)
            acc[at, :] += gate * jnp.dot(pick, rows[...], preferred_element_type=F32)
            return c
        lax.fori_loop(0, tiles, body, 0)

    def hot_gate(i, c):
        at = pl.ds(pl.multiple_of(i * tile, tile), tile)
        tok = lax.broadcasted_iota(jnp.int32, (tile, hot_tok_ref.shape[1]), 0) + i * tile
        hot_w[at, :] = jnp.sum(jnp.where(hot_tok_ref[...] == tok, hot_g_ref[...], 0.0), axis=1, keepdims=True)
        acc[at, :] = jnp.zeros((tile, d_model), F32)
        return c
    lax.fori_loop(0, tiles, hot_gate, 0)

    @pl.when(me != 0)
    def _():
        combine(me, hbuf.at[0])

    def combine_step(t, c):
        @pl.when(t == HOT_SHARE)
        def _():
            for leg in LEG2:
                s2_copy(*leg, arriving=True).wait_recv()
            for leg in LEG1 + LEG2:
                s2_copy(*leg).wait_send()
            s3_copy(core).start()

        @pl.when(t == HOT_RUN)
        def _():
            s3_copy(core).wait_send()
            s3_copy(1 - core).wait_recv()

            def hot_step(i, c):
                at = pl.ds(pl.multiple_of(i * tile, tile), tile)
                acc[at, :] += hot_w[at, :] * swiglu(x_ref[at, :], hot).astype(F32)
                return c
            lax.fori_loop(0, tiles, hot_step, 0)

        dx, dy, dc = place_of(ARRIVALS, t)
        q = slot_of(dx, dy, dc)
        for axis in (0, 1):
            through, steps = across(axis, dx, dy, dc)

            @pl.when((through != 0) & (steps != 0))
            def _():
                back2(axis, dx, dy, dc).wait_send()
        maker = dev(dx, dy, dc)

        @pl.when(maker != 0)
        def _():
            for axis in (0, 1):
                _, steps = across(axis, dx, dy, dc)

                @pl.when(steps != 0)
                def _():
                    back2(axis, dx, dy, dc).wait_recv()

                @pl.when(steps == 0)
                def _():
                    hbuf[q, :, cols[axis]] = xbuf[q, :, cols[axis]]
            combine(maker, hbuf.at[q])
        return c
    lax.fori_loop(1, n, combine_step, 0)

    @pl.when(me == 0)
    def _():
        def sent(d, c):
            s1_copy(d).wait_send()
            return c
        lax.fori_loop(1, n, sent, 0)

    def out_copy(axis, i):
        at = pl.ds(pl.multiple_of(i * tile, tile), tile)
        return pltpu.make_async_copy(rings[axis].at[0, at, :], out_ref.at[at, cols[axis]], out_sem.at[axis, i])

    for i in range(tiles):
        for axis in (0, 1):
            rings[axis][0, pl.ds(i * tile, tile), :] = acc[pl.ds(i * tile, tile), cols[axis]].astype(BF16)
            if i:
                out_copy(axis, i - 1).start()
    for axis in (0, 1):
        out_copy(axis, tiles - 1).start()
    for i in range(tiles):
        for axis in (0, 1):
            out_copy(axis, i).wait()


def solution(mesh):
    n = mesh.shape['ep']
    row_spec = P(('dp', 'ep'), None)
    list_spec = P(('dp', 'ep'))
    expert_spec = P('ep', None, None)

    def local_layer(x, ids, gates, hot_tok, hot_g, wg, wu, wd):
        tokens, d_model = x.shape
        top_k = ids.shape[1]
        d_ff = wg.shape[2]
        cap = (tokens * top_k + n - 2) // (n - 1)
        cap_p = -(-cap // 16) * 16
        lanes = -(-n // 128) * 128
        half = n // 2
        vmem = pl.BlockSpec(memory_space=pltpu.VMEM)
        hbm = pl.BlockSpec(memory_space=pltpu.HBM)
        dma = pltpu.SemaphoreType.DMA
        return pl.pallas_call(
            functools.partial(moe_kernel, n, cap_p),
            out_shape=jax.ShapeDtypeStruct((tokens, d_model), BF16),
            in_specs=[vmem] * 5 + [hbm] * 3,
            out_specs=hbm,
            scratch_shapes=[
                pltpu.VMEM((d_model + d_ff, d_model), BF16),
                pltpu.VMEM((d_model + d_ff, d_model), BF16),
                pltpu.VMEM((n, cap_p, d_model), BF16),
                pltpu.VMEM((n, cap_p, d_model), BF16),
                pltpu.VMEM((SIDE - 1, tokens, d_model // 2), BF16),
                pltpu.VMEM((SIDE - 1, tokens, d_model // 2), BF16),
                pltpu.VMEM((SIDE, 2 * SIDE, tokens), F32),
                pltpu.VMEM((SIDE, 2 * SIDE, tokens), F32),
                pltpu.VMEM((tokens, lanes), F32),
                pltpu.VMEM((tokens, lanes), F32),
                pltpu.VMEM((lanes, tokens), F32),
                pltpu.VMEM((n, tokens), F32),
                pltpu.VMEM((tokens, 1), F32),
                pltpu.VMEM((tokens, d_model), F32),
                dma((3,)), dma((n,)), dma, dma((2, half - 1)), dma((2, half - 1)), dma, dma,
                dma((2, SIDE)), dma((2, SIDE)), dma((2, SIDE)), dma((2, SIDE)),
                dma((2, n)), dma((2, n)), dma((2, n)), dma((2, n)), dma((2, n)), dma((2, n)), dma((2, tokens // 256)),
                pltpu.SemaphoreType.REGULAR((2, n)), pltpu.SemaphoreType.REGULAR((2, n)),
            ],
            compiler_params=pltpu.CompilerParams(
                collective_id=0, has_side_effects=True, vmem_limit_bytes=67_043_328),
        )(x, ids.T, gates.T, hot_tok.reshape(1, -1), hot_g.reshape(1, -1), wg, wu, wd)

    return jax.shard_map(local_layer, mesh=mesh,
                         in_specs=(row_spec, row_spec, row_spec, list_spec, list_spec, expert_spec, expert_spec, expert_spec),
                         out_specs=row_spec, check_vma=False)
```

```python
import functools

import jax
import jax.numpy as jnp
from jax import lax
from jax.experimental import pallas as pl
from jax.experimental.pallas import tpu as pltpu
from jax.sharding import PartitionSpec as P

MESH = pl.DeviceIdType.MESH
F32 = jnp.float32
BF16 = jnp.bfloat16
OFFSETS = ((0, 0), (1, 1), (3, 3), (1, 3), (3, 1), (2, 2), (1, 2), (3, 2), (2, 1), (2, 3),
           (1, 0), (3, 0), (0, 1), (0, 3), (2, 0), (0, 2))
SIDE = 4
RING = (0, 1, 3, 2)
ARRIVALS = ((0, 0), (1, 0), (0, 1), (3, 0), (0, 3), (1, 1), (2, 0), (0, 2), (1, 3), (3, 1), (3, 3), (2, 1), (1, 2), (2, 3), (3, 2), (2, 2))
HOT_LEG = 12
HOT_SHARE = 10
HOT_RUN = 16


def packed(values):
    return sum(v << (2 * i) for i, v in enumerate(values))


def entry(table, i):
    return lax.rem(lax.shift_right_logical(jnp.int32(table), 2 * i), SIDE)


def place_of(order, t):
    j = lax.div(t, 2)
    i = lax.max(j - 1, 0)
    near = lax.min(j, 1)
    dx = entry(packed([o[0] for o in order[1:]]), i) * near
    dy = entry(packed([o[1] for o in order[1:]]), i) * near
    return dx, dy, lax.rem(t, 2)


def moe_kernel(n, cap_p, x_hbm, ids_ref, gates_ref, hot_tok_ref, hot_g_ref, wg_ref, wu_ref, wd_ref, out_ref,
               x_ref, own, hot, xbuf, hbuf, ring_x, ring_y, tab_x, tab_y, slot_t, gate_t, slot_r, slot_x, hot_w, acc,
               w_sem, s1_send, s1_recv, s2_send, s2_recv, s3_send, s3_recv,
               rows_send, rows_recv, tabs_send, tabs_recv, part_send, part_recv, h1_send, h1_recv, h2_send, h2_recv, out_sem, free, ready):
    tokens, d_model = x_ref.shape
    top_k = ids_ref.shape[0]
    d_ff = wg_ref.shape[2]
    lanes = slot_t.shape[1]
    chunk = own.shape[0] // n
    half = n // 2
    wide = d_model // 2
    me = lax.axis_index('ep')
    core = lax.rem(me, 2)
    chip = lax.div(me, 2)
    px = lax.rem(chip, SIDE)
    py = lax.div(chip, SIDE)

    def dev(dx, dy, dc):
        tx = lax.rem(px + dx + SIDE, SIDE)
        ty = lax.rem(py + dy + SIDE, SIDE)
        return (ty * SIDE + tx) * 2 + lax.rem(core + dc, 2)

    def slot_of(dx, dy, dc):
        return (dy * SIDE + dx) * 2 + dc

    def remote(src, dst, send, recv, device):
        return pltpu.make_async_remote_copy(src_ref=src, dst_ref=dst, send_sem=send, recv_sem=recv,
                                            device_id={'ep': device}, device_id_type=MESH)

    x_in = pltpu.make_async_copy(x_hbm, x_ref, w_sem.at[3])
    x_in.start()
    barrier = pltpu.get_barrier_semaphore()

    def greet(k, c):
        pl.semaphore_signal(barrier, inc=1, device_id={'ep': lax.rem(me + k, n)}, device_id_type=MESH)
        return c
    lax.fori_loop(1, n, greet, 0)

    w_copies = (
        pltpu.make_async_copy(wg_ref.at[0], own.at[pl.ds(0, d_model), pl.ds(0, d_ff)], w_sem.at[0]),
        pltpu.make_async_copy(wu_ref.at[0], own.at[pl.ds(0, d_model), pl.ds(d_ff, d_ff)], w_sem.at[1]),
        pltpu.make_async_copy(wd_ref.at[0], own.at[pl.ds(d_model, d_ff), :], w_sem.at[2]),
    )
    pl.semaphore_wait(barrier, n - 1)
    x_in.wait()

    cols = (pl.ds(0, wide), pl.ds(wide, wide))
    rings = (ring_x, ring_y)
    tabs = (tab_x, tab_y)

    def step_of(axis, a):
        return dev(a, 0, 0) if axis == 0 else dev(0, a, 0)

    def rows_copy(axis, a):
        return remote(x_ref.at[:, cols[axis]], rings[axis].at[a - 1], rows_send.at[axis, a], rows_recv.at[axis, a],
                      step_of(axis, a))

    def tabs_copy(axis, a):
        if axis == 0:
            src = slot_x.at[pl.ds(pl.multiple_of(lax.rem(px + a, SIDE) * 8, 8), 8), :]
        else:
            src = slot_r.at[pl.ds(pl.multiple_of(lax.rem(py + a, SIDE) * 8, 8), 8), :]
        return remote(src, tabs[axis].at[a], tabs_send.at[axis, a], tabs_recv.at[axis, a], step_of(axis, a))

    def rows_onward(axis, ahead):
        at = pl.ds(0 if ahead else tokens // 2, tokens // 2)
        ring = rings[axis]
        i = 2 if ahead else 0
        return remote(ring.at[0 if ahead else 2, at, :], ring.at[1, at, :], rows_send.at[axis, i],
                      rows_recv.at[axis, i], step_of(axis, 1 if ahead else -1))

    for a in (1, 3):
        for axis in (0, 1):
            rows_copy(axis, a).start()

    for copy in w_copies:
        copy.start()

    expert = lax.broadcasted_iota(jnp.int32, (lanes, tokens), 0)
    chosen = jnp.zeros((lanes, tokens), F32)
    gate_sum = jnp.zeros((lanes, tokens), F32)
    for j in range(top_k):
        hit = ids_ref[pl.ds(j, 1), :] == expert
        chosen = jnp.where(hit, 1.0, chosen)
        gate_sum = jnp.where(hit, gates_ref[pl.ds(j, 1), :], gate_sum)
    gate_t[...] = gate_sum.T
    chosen_b = chosen.astype(BF16)
    step = 256
    for r in range(tokens // step):
        upto = lax.broadcasted_iota(jnp.int32, (tokens, step), 1) + r * step
        before = jnp.where(lax.broadcasted_iota(jnp.int32, (tokens, step), 0) < upto, 1.0, 0.0).astype(BF16)
        rank = jnp.dot(chosen_b, before, preferred_element_type=F32)
        slot_r[:, pl.ds(r * step, step)] = jnp.where(chosen[:, r * step:(r + 1) * step] > 0.5, rank, -1.0)
    slot_t[...] = slot_r[...].T
    for tx in range(SIDE):
        for ty in range(SIDE):
            slot_x[pl.ds(tx * 8 + ty * 2, 2), :] = slot_r[pl.ds((ty * SIDE + tx) * 2, 2), :]
    tab_x[0] = slot_x[pl.ds(pl.multiple_of(px * 8, 8), 8), :]
    tab_y[0] = slot_r[pl.ds(pl.multiple_of(py * 8, 8), 8), :]
    for a in RING[1:]:
        for axis in (0, 1):
            tabs_copy(axis, a).start()

    def part(axis, a, m):
        b = entry(packed(RING[1:] + RING[:1]), lax.div(m, 2))
        dc = lax.rem(m, 2)
        q = slot_of(a, b, dc) if axis == 0 else slot_of(b, a, dc)
        target = dev(0, b, dc) if axis == 0 else dev(b, 0, dc)
        row = lax.rem((py if axis == 0 else px) + b, SIDE) * 2 + lax.rem(core + dc, 2)
        return q, target, row

    def part_copy(axis, q, target):
        return remote(xbuf.at[q, :, cols[axis]], hbuf.at[q, :, cols[axis]], part_send.at[axis, q],
                      part_recv.at[axis, q], target)

    pos = lax.broadcasted_iota(jnp.int32, (cap_p, tokens), 0).astype(F32)

    def gather(axis, a, m):
        q, target, row = part(axis, a, m)

        @pl.when(target != 0)
        def _():
            source = x_ref[:, cols[axis]] if a == 0 else rings[axis][a - 1]
            pick = jnp.where(pos == tabs[axis][a, pl.ds(row, 1), :], 1.0, 0.0).astype(BF16)
            xbuf[q, :, cols[axis]] = jnp.dot(pick, source, preferred_element_type=F32).astype(BF16)

    def post(axis, a, m):
        q, target, row = part(axis, a, m)

        @pl.when((target != 0) & (target != me))
        def _():
            part_copy(axis, q, target).start()

        @pl.when((target != 0) & (target == me))
        def _():
            hbuf[q, :, cols[axis]] = xbuf[q, :, cols[axis]]

    for a in RING:
        for axis in (0, 1):
            if a == 1:
                for b in (1, 3):
                    rows_copy(axis, b).wait_recv()
                    rows_onward(axis, b == 1).start()
            if a == 2:
                for ahead in (True, False):
                    rows_onward(axis, ahead).wait_recv()
            if a:
                tabs_copy(axis, a).wait_recv()

        def gather_step(m, c, a=a):
            gather(0, a, m)

            @pl.when(m > 0)
            def _():
                post(1, a, m - 1)
            gather(1, a, m)
            post(0, a, m)
            return c
        lax.fori_loop(0, 2 * SIDE, gather_step, 0)
        post(1, a, jnp.int32(2 * SIDE - 1))

    for axis in (0, 1):
        for a in (1, 3):
            rows_copy(axis, a).wait_send()
            rows_onward(axis, a == 1).wait_send()
        for a in RING[1:]:
            tabs_copy(axis, a).wait_send()
    for copy in w_copies:
        copy.wait()

    def swiglu(rows, weights):
        mid = jnp.dot(rows, weights[pl.ds(0, d_model), :], preferred_element_type=F32)
        a = mid[:, :d_ff]
        u = (a * jax.nn.sigmoid(a) * mid[:, d_ff:]).astype(BF16)
        return jnp.dot(u, weights[pl.ds(d_model, d_ff), :], preferred_element_type=F32).astype(BF16)

    def back1(axis, dx, dy, dc):
        q = slot_of(dx, dy, dc)
        relay = dev(0, -dy, dc) if axis == 0 else dev(-dx, 0, dc)
        return relay, remote(hbuf.at[q, :, cols[axis]], xbuf.at[q, :, cols[axis]], h1_send.at[axis, q],
                             h1_recv.at[axis, q], relay)

    def back2(axis, dx, dy, dc):
        q = slot_of(dx, dy, dc)
        source = dev(-dx, 0, 0) if axis == 0 else dev(0, -dy, 0)
        return remote(xbuf.at[q, :, cols[axis]], hbuf.at[q, :, cols[axis]], h2_send.at[axis, q],
                      h2_recv.at[axis, q], source)

    def across(axis, dx, dy, dc):
        return (dev(0, dy, dc), dx) if axis == 0 else (dev(dx, 0, dc), dy)

    def send_back(t):
        dx, dy, dc = place_of(ARRIVALS, t)
        q = slot_of(dx, dy, dc)
        for axis in (0, 1):
            relay, copy = back1(axis, dx, dy, dc)

            @pl.when((me != 0) & (relay != me))
            def _():
                pl.semaphore_wait(free.at[axis, q], 1)
                copy.start()

            @pl.when((me != 0) & (relay == me))
            def _():
                xbuf[q, :, cols[axis]] = hbuf[q, :, cols[axis]]

    def expert_step(t, c):
        dx, dy, dc = place_of(ARRIVALS, t)
        q = slot_of(dx, dy, dc)
        for axis in (0, 1):
            target, _ = across(axis, dx, dy, dc)

            @pl.when((target != 0) & (target != me))
            def _():
                part_copy(axis, q, target).wait_send()
                pl.semaphore_signal(free.at[axis, q], inc=1, device_id={'ep': target}, device_id_type=MESH)

        @pl.when(me != 0)
        def _():
            for axis in (0, 1):
                target, _ = across(axis, dx, dy, dc)

                @pl.when(target != me)
                def _():
                    part_copy(axis, q, target).wait_recv()
            hbuf[q] = swiglu(hbuf[q], own)

        @pl.when(t > 1)
        def _():
            send_back(t - 1)
        return c

    def piece(d):
        return pl.ds(pl.multiple_of((lax.rem(d, 2) * half + lax.div(d, 2)) * chunk, chunk), chunk)

    def s1_copy(d):
        return remote(own.at[piece(d), :], hot.at[piece(d), :], s1_send.at[d], s1_recv, d)

    def s2_copy(axis, a, b, arriving=False):
        first = a is None
        if first:
            peer = step_of(axis, -b if arriving else b)
            held = piece(peer if arriving else me)
            i = b - 1
        else:
            back = b if arriving else 0
            held = piece(dev(-a, -back, 0) if axis == 0 else dev(-back, -a, 0))
            peer = step_of(1 - axis, -b if arriving else b)
            i = SIDE - 1 + a * (SIDE - 1) + b - 1
        at = hot.at[held, cols[axis]]
        return remote(at, at, s2_send.at[axis, i], s2_recv.at[axis, i], peer)

    LEG1 = [(axis, None, b) for b in RING[1:] for axis in (0, 1)]
    LEG2 = [(axis, a, b) for a in RING for b in RING[1:] for axis in (0, 1)]

    def core_half(c):
        return hot.at[pl.ds(pl.multiple_of(c * half * chunk, chunk), half * chunk), :]

    def s3_copy(c):
        return remote(core_half(c), core_half(c), s3_send, s3_recv, dev(0, 0, 1))

    @pl.when(me == 0)
    def _():
        hot[pl.ds(0, chunk), :] = own[pl.ds(0, chunk), :]

        def send(t, c):
            dx, dy, dc = place_of(OFFSETS, t)
            s1_copy(dev(dx, dy, dc)).start()
            return c
        lax.fori_loop(1, n, send, 0)

    lax.fori_loop(0, n, expert_step, 0)
    send_back(jnp.int32(n - 1))

    @pl.when(me != 0)
    def _():
        s1_copy(me).wait_recv()
    for leg in LEG1:
        s2_copy(*leg).start()

    def forward(t):
        dx, dy, dc = place_of(ARRIVALS, t)
        q = slot_of(dx, dy, dc)
        for axis in (0, 1):
            maker, steps = across(axis, dx, dy, dc)

            @pl.when((maker != 0) & (maker != me))
            def _():
                back1(axis, dx, dy, dc)[1].wait_recv()

            @pl.when((maker != 0) & (steps != 0))
            def _():
                pl.semaphore_wait(ready.at[axis, q], 1)
                back2(axis, dx, dy, dc).start()

    def relay_step(t, c):
        @pl.when(t == HOT_LEG)
        def _():
            for leg in LEG1:
                s2_copy(*leg, arriving=True).wait_recv()
            for leg in LEG2:
                s2_copy(*leg).start()

        dx, dy, dc = place_of(ARRIVALS, t)
        q = slot_of(dx, dy, dc)
        for axis in (0, 1):
            relay, copy = back1(axis, dx, dy, dc)

            @pl.when((me != 0) & (relay != me))
            def _():
                copy.wait_send()
            _, steps = across(axis, dx, dy, dc)
            via = dev(dx, 0, 0) if axis == 0 else dev(0, dy, 0)

            @pl.when((steps != 0) & (dev(dx, dy, dc) != 0))
            def _():
                pl.semaphore_signal(ready.at[axis, q], inc=1, device_id={'ep': via}, device_id_type=MESH)

        @pl.when(t > 1)
        def _():
            forward(t - 1)
        return c
    lax.fori_loop(1, n, relay_step, 0)
    forward(jnp.int32(n - 1))

    tile = 256
    tiles = tokens // tile
    own_lane = lax.broadcasted_iota(jnp.int32, (tile, lanes), 1)
    pos_lane = lax.broadcasted_iota(jnp.int32, (tile, cap_p), 1).astype(F32)

    def weighted(e, rows, at):
        mine = own_lane == e
        place = jnp.sum(jnp.where(mine, slot_t[at, :], 0.0), axis=1, keepdims=True)
        gate = jnp.sum(jnp.where(mine, gate_t[at, :], 0.0), axis=1, keepdims=True)
        pick = jnp.where(pos_lane == place, 1.0, 0.0).astype(BF16)
        acc[at, :] += gate * jnp.dot(pick, rows[...], preferred_element_type=F32)

    def combine(e, rows):
        def body(i, c):
            weighted(e, rows, pl.ds(pl.multiple_of(i * tile, tile), tile))
            return c
        lax.fori_loop(0, tiles, body, 0)

    def hot_gate(i, c):
        at = pl.ds(pl.multiple_of(i * tile, tile), tile)
        tok = lax.broadcasted_iota(jnp.int32, (tile, hot_tok_ref.shape[1]), 0) + i * tile
        hot_w[at, :] = jnp.sum(jnp.where(hot_tok_ref[...] == tok, hot_g_ref[...], 0.0), axis=1, keepdims=True)
        acc[at, :] = jnp.zeros((tile, d_model), F32)
        return c
    lax.fori_loop(0, tiles, hot_gate, 0)

    @pl.when(me != 0)
    def _():
        combine(me, hbuf.at[0])

    def combine_step(t, c):
        @pl.when(t == HOT_SHARE)
        def _():
            for leg in LEG2:
                s2_copy(*leg, arriving=True).wait_recv()
            for leg in LEG1 + LEG2:
                s2_copy(*leg).wait_send()
            s3_copy(core).start()

        @pl.when(t == HOT_RUN)
        def _():
            s3_copy(core).wait_send()
            s3_copy(1 - core).wait_recv()

            def hot_step(i, c):
                at = pl.ds(pl.multiple_of(i * tile, tile), tile)
                acc[at, :] += hot_w[at, :] * swiglu(x_ref[at, :], hot).astype(F32)
                return c
            lax.fori_loop(0, tiles, hot_step, 0)

        dx, dy, dc = place_of(ARRIVALS, t)
        q = slot_of(dx, dy, dc)
        for axis in (0, 1):
            through, steps = across(axis, dx, dy, dc)

            @pl.when((through != 0) & (steps != 0))
            def _():
                back2(axis, dx, dy, dc).wait_send()
        maker = dev(dx, dy, dc)

        @pl.when(maker != 0)
        def _():
            for axis in (0, 1):
                _, steps = across(axis, dx, dy, dc)

                @pl.when(steps != 0)
                def _():
                    back2(axis, dx, dy, dc).wait_recv()

                @pl.when(steps == 0)
                def _():
                    hbuf[q, :, cols[axis]] = xbuf[q, :, cols[axis]]

            @pl.when(t < n - 1)
            def _():
                combine(maker, hbuf.at[q])
        return c
    lax.fori_loop(1, n, combine_step, 0)
    final = place_of(ARRIVALS, jnp.int32(n - 1))

    @pl.when(me == 0)
    def _():
        def sent(d, c):
            s1_copy(d).wait_send()
            return c
        lax.fori_loop(1, n, sent, 0)

    def out_copy(axis, i):
        at = pl.ds(pl.multiple_of(i * tile, tile), tile)
        return pltpu.make_async_copy(rings[axis].at[0, at, :], out_ref.at[at, cols[axis]], out_sem.at[axis, i])

    for i in range(tiles):
        @pl.when(dev(*final) != 0)
        def _():
            weighted(dev(*final), hbuf.at[slot_of(*final)], pl.ds(i * tile, tile))
        for axis in (0, 1):
            rings[axis][0, pl.ds(i * tile, tile), :] = acc[pl.ds(i * tile, tile), cols[axis]].astype(BF16)
            if i:
                out_copy(axis, i - 1).start()
    for axis in (0, 1):
        out_copy(axis, tiles - 1).start()
    for i in range(tiles):
        for axis in (0, 1):
            out_copy(axis, i).wait()


def solution(mesh):
    n = mesh.shape['ep']
    row_spec = P(('dp', 'ep'), None)
    list_spec = P(('dp', 'ep'))
    expert_spec = P('ep', None, None)

    def local_layer(x, ids, gates, hot_tok, hot_g, wg, wu, wd):
        tokens, d_model = x.shape
        top_k = ids.shape[1]
        d_ff = wg.shape[2]
        cap = (tokens * top_k + n - 2) // (n - 1)
        cap_p = -(-cap // 16) * 16
        lanes = -(-n // 128) * 128
        half = n // 2
        vmem = pl.BlockSpec(memory_space=pltpu.VMEM)
        hbm = pl.BlockSpec(memory_space=pltpu.HBM)
        dma = pltpu.SemaphoreType.DMA
        return pl.pallas_call(
            functools.partial(moe_kernel, n, cap_p),
            out_shape=jax.ShapeDtypeStruct((tokens, d_model), BF16),
            in_specs=[hbm] + [vmem] * 4 + [hbm] * 3,
            out_specs=hbm,
            scratch_shapes=[
                pltpu.VMEM((tokens, d_model), BF16),
                pltpu.VMEM((d_model + d_ff, d_model), BF16),
                pltpu.VMEM((d_model + d_ff, d_model), BF16),
                pltpu.VMEM((n, cap_p, d_model), BF16),
                pltpu.VMEM((n, cap_p, d_model), BF16),
                pltpu.VMEM((SIDE - 1, tokens, d_model // 2), BF16),
                pltpu.VMEM((SIDE - 1, tokens, d_model // 2), BF16),
                pltpu.VMEM((SIDE, 2 * SIDE, tokens), F32),
                pltpu.VMEM((SIDE, 2 * SIDE, tokens), F32),
                pltpu.VMEM((tokens, lanes), F32),
                pltpu.VMEM((tokens, lanes), F32),
                pltpu.VMEM((lanes, tokens), F32),
                pltpu.VMEM((n, tokens), F32),
                pltpu.VMEM((tokens, 1), F32),
                pltpu.VMEM((tokens, d_model), F32),
                dma((4,)), dma((n,)), dma, dma((2, half - 1)), dma((2, half - 1)), dma, dma,
                dma((2, SIDE)), dma((2, SIDE)), dma((2, SIDE)), dma((2, SIDE)),
                dma((2, n)), dma((2, n)), dma((2, n)), dma((2, n)), dma((2, n)), dma((2, n)), dma((2, tokens // 256)),
                pltpu.SemaphoreType.REGULAR((2, n)), pltpu.SemaphoreType.REGULAR((2, n)),
            ],
            compiler_params=pltpu.CompilerParams(
                collective_id=0, has_side_effects=True, vmem_limit_bytes=67_043_328),
        )(x, ids.T, gates.T, hot_tok.reshape(1, -1), hot_g.reshape(1, -1), wg, wu, wd)

    return jax.shard_map(local_layer, mesh=mesh,
                         in_specs=(row_spec, row_spec, row_spec, list_spec, list_spec, expert_spec, expert_spec, expert_spec),
                         out_specs=row_spec, check_vma=False)
```
